256 devices in a mesh: groups: 2 (over y), gx: 32 (over z, core), gy: 4 (over x).
Axes of the slice: x: 4, y: 2, z: 16, core: 2. Of those that a mesh axis runs over, the one named last changes fastest.
The devices are a block of a 4x16x16 slice.
Arguments:
- initial_state: float32 [64, 4, 65536], P(('groups', 'gx'), 'gy'), parts along dimension 0, may hold values from -80 to 80
- fields: float32 [46], P('groups'), parts along dimension 0, may hold values from -3 to 3
- bond_order: int32 [4, 6], replicated, may hold values from 0 to 5, each once within a row
Outputs:
- amplitudes: float32 [64, 4, 65536], P(('groups', 'gx'), 'gy'), parts along dimension 0
The draws below stay inside these ranges and needn't reach their ends.
There are 2 independent parts, one for each index of `groups`. The reference program is written for one: setup_inputs(seed, part) draws one part's arguments, and reference() takes and returns one part's arrays. A program takes and returns all parts, laid end to end along the dimension named above; an argument that names none is the same for every part. Nothing has to cross between parts.
Inputs may be any that keep to these rules, and one draw needn't show every extreme that they name: `bond_order`: each row is an ordering of the six bonds of its window; entry e names the bond between sites s_w + e and s_w + e + 1.
All inputs are finite; a program needn't handle non-finite values.
Results may differ from the reference program's by a relative error of at most 0.0001.
Values sent between devices are 32-bit elements; how exact they have to be, the bound alone decides.
A program may use at most 64 MiB of HBM per device.

```python
import jax
import jax.numpy as jnp
from jax import lax

AMPS = 65536
WINDOWS = 4
LOCAL = 16
SITES = 23
TOTAL = 8388608
N_GX = 32
N_GY = 4


def draw_initial_state(key, part):
    first_key, second_key = jax.random.split(jax.random.fold_in(key, 11))
    position = jnp.arange(TOTAL, dtype=jnp.float32) / TOTAL
    blocks = jax.random.uniform(second_key, (TOTAL // 128, 1), jnp.float32)
    rough = jnp.broadcast_to(blocks, (TOTAL // 128, 128)).reshape(-1)
    values = jnp.clip(jax.random.normal(first_key, (TOTAL,), jnp.float32), -5.0, 5.0)
    scale = 10.0 ** (0.6 * position + 0.5 * rough)
    return (values * scale).reshape(N_GX, N_GY, AMPS)


def setup_inputs(seed: int = 0, part: int = 0) -> dict:
    keys = jax.random.split(jax.random.key(seed), 4)
    part_splits = jax.random.split(jax.random.fold_in(keys[3], part), 4)
    initial_state = draw_initial_state(jax.random.fold_in(jax.random.fold_in(keys[3], part), 71), part)
    fields = jnp.clip(jax.random.uniform(part_splits[1], (SITES,), jnp.float32, -3.0, 3.0), -3.0, 3.0)
    bond_order = jax.vmap(lambda own: jax.random.permutation(own, 6))(jax.random.split(keys[2], WINDOWS)).reshape((WINDOWS, 6)).astype(jnp.int32)
    return dict(initial_state=initial_state, fields=fields, bond_order=bond_order)


coupling = 1.0
step_time = 0.15
epsilon = 1e-06
HIGHEST = lax.Precision.HIGHEST

def make_gates(fields):
    left_field = fields[:-1]
    right_field = fields[1:]
    half_sum = 0.5 * (left_field + right_field)
    half_diff = 0.5 * (left_field - right_field)
    radius = jnp.sqrt(half_diff * half_diff + 4.0 * coupling * coupling)
    boosted = jnp.exp(step_time * coupling) * jnp.ones_like(half_sum)
    cosine = jnp.cosh(step_time * radius)
    sine_ratio = jnp.sinh(step_time * radius) / radius
    corner_low = jnp.exp(-step_time * (coupling + half_sum))
    corner_high = jnp.exp(-step_time * (coupling - half_sum))
    middle_up = boosted * (cosine - sine_ratio * half_diff)
    middle_down = boosted * (cosine + sine_ratio * half_diff)
    flipping = -2.0 * coupling * boosted * sine_ratio
    nothing = jnp.zeros_like(half_sum)
    entries = [corner_low, nothing, nothing, nothing, nothing, middle_up, flipping, nothing, nothing, flipping, middle_down, nothing, nothing, nothing, nothing, corner_high]
    return jnp.stack(entries, axis=1).reshape(-1, 4, 4)

def pair_apply(matrix, gate, first_bit, second_bit, count_bits):
    tensor = gate.reshape(2, 2, 2, 2)
    shaped = matrix.reshape((2,) * count_bits + (matrix.shape[1],))
    axis_first = count_bits - 1 - first_bit
    axis_second = count_bits - 1 - second_bit
    moved = jnp.tensordot(tensor, shaped, axes=([2, 3], [axis_first, axis_second]), precision=HIGHEST)
    return jnp.moveaxis(moved, [0, 1], [axis_first, axis_second]).reshape(matrix.shape)

def window_start(position, local_bits):
    return (0, 7, local_bits - 7, 1)[position % 4]

def window_matrix(bond_gates, order_row, start_bit):
    identity = jnp.eye(128, dtype=bond_gates.dtype)
    singles = [pair_apply(identity, bond_gates[start_bit + offset], offset, offset + 1, 7) for offset in range(6)]
    matrix = identity
    for section_number in range(6):
        chosen = jnp.zeros_like(identity)
        for offset in range(6):
            chosen = chosen + (order_row[section_number] == offset).astype(identity.dtype) * singles[offset]
        matrix = jnp.dot(chosen, matrix, precision=HIGHEST)
    return matrix

def apply_window(vector, matrix, start_bit):
    if start_bit == 0:
        shaped = vector.reshape(-1, 128)
        return jnp.dot(shaped, matrix.T, precision=HIGHEST).reshape(-1)
    if start_bit == 1:
        widened = jnp.kron(matrix, jnp.eye(2, dtype=matrix.dtype))
        shaped = vector.reshape(-1, 256)
        return jnp.dot(shaped, widened.T, precision=HIGHEST).reshape(-1)
    shaped = vector.reshape(-1, 128, 2 ** start_bit)
    return jnp.einsum('hg,agb->ahb', matrix, shaped, precision=HIGHEST).reshape(-1)

def evolve_windows(vector, bond_gates, bond_order, local_bits):

    def one_cycle(cycle_number, current):
        for position in range(4):
            start_bit = window_start(position, local_bits)
            order_row = lax.dynamic_index_in_dim(bond_order, 4 * cycle_number + position, 0, keepdims=False)
            current = apply_window(current, window_matrix(bond_gates, order_row, start_bit), start_bit)
        return current
    return lax.fori_loop(0, bond_order.shape[0] // 4, one_cycle, vector)

def apply_bond(vector, gate, site_index, total_sites):
    shaped = vector.reshape(2 ** (total_sites - site_index - 2), 2, 2, 2 ** site_index)
    tensor = gate.reshape(2, 2, 2, 2)
    return jnp.einsum('xyab,pbaq->pyxq', tensor, shaped, precision=HIGHEST).reshape(-1)

def reference(initial_state, fields, bond_order):
    bond_gates = make_gates(fields)
    vector = evolve_windows(initial_state.reshape(-1), bond_gates, bond_order, LOCAL)
    for site_index in range(LOCAL - 1, SITES - 1):
        vector = apply_bond(vector, bond_gates[site_index], site_index, SITES)
    mean_square = jnp.sum(vector * vector) / TOTAL
    scaled = vector * lax.rsqrt(mean_square + epsilon)
    return scaled.reshape(initial_state.shape)
```

```python
import functools

import jax
import jax.numpy as jnp
from jax import lax
from jax.experimental import pallas as pl
from jax.experimental.pallas import tpu as pltpu
from jax.sharding import PartitionSpec as P

MESH = pl.DeviceIdType.MESH
STEP = 0.15
BOOST = 1.161834242728283
EPSILON = 1e-06
STARTS = (0, 7, 9, 1)


def gate_entries(left, right, shape):
    left = jnp.full(shape, left, jnp.float32)
    right = jnp.full(shape, right, jnp.float32)
    half_sum = 0.5 * (left + right)
    half_diff = 0.5 * (left - right)
    radius = jnp.sqrt(half_diff * half_diff + 4.0)
    grow = jnp.exp(STEP * radius)
    decay = jnp.exp(-STEP * radius)
    cosine = 0.5 * (grow + decay)
    sine_ratio = 0.5 * (grow - decay) / radius
    low = jnp.exp(-STEP * (1.0 + half_sum))
    high = jnp.exp(-STEP * (1.0 - half_sum))
    up = BOOST * (cosine - sine_ratio * half_diff)
    down = BOOST * (cosine + sine_ratio * half_diff)
    flip = -2.0 * BOOST * sine_ratio
    return low, up, down, high, flip


def bond_step(matrix, fields, start, offset, lane):
    low, up, down, high, flip = gate_entries(
        fields[start + offset], fields[start + offset + 1], lane.shape
    )
    first = (lane >> offset) & 1
    second = (lane >> (offset + 1)) & 1
    zero = first == 0
    equal = first == second
    diagonal = jnp.where(equal, jnp.where(zero, low, high), jnp.where(zero, up, down))
    from_below = jnp.where(equal, 0.0, jnp.where(zero, flip, 0.0))
    from_above = jnp.where(equal, 0.0, jnp.where(zero, 0.0, flip))
    shift = jnp.left_shift(1, offset)
    return (
        matrix * diagonal
        + pltpu.roll(matrix, shift, 1) * from_below
        + pltpu.roll(matrix, 128 - shift, 1) * from_above
    )


def split(x):
    high = x.astype(jnp.bfloat16)
    return high, (x - high.astype(jnp.float32)).astype(jnp.bfloat16)


def dot(a, b):
    return jnp.dot(a, b, preferred_element_type=jnp.float32)


def dot_split(a, b):
    return dot(a[0], b[0]) + (dot(a[0], b[1]) + dot(a[1], b[0]))


def mix(value, entries, bit):
    low, up, down, high, flip = entries
    rows = value.shape[0]
    inner = 2**bit
    v = value.reshape(rows // (4 * inner), 2, 2, inner // 8, 8, 128)
    both0, only_first = v[:, 0, 0], v[:, 0, 1]
    only_second, both1 = v[:, 1, 0], v[:, 1, 1]
    new = jnp.stack(
        [
            jnp.stack([low * both0, down * only_first + flip * only_second], axis=1),
            jnp.stack([up * only_second + flip * only_first, high * both1], axis=1),
        ],
        axis=1,
    )
    return new.reshape(value.shape)


def kernel(
    x_ref,
    fields,
    order,
    o_ref,
    t_ref,
    send,
    held,
    back,
    final,
    part_z,
    part_xc,
    got_z,
    got_xc,
    send_sems,
    recv_sems,
    got_z_sem,
    got_xc_sem,
):
    gx, gy = lax.axis_index("gx"), lax.axis_index("gy")
    n_z, n_x = lax.axis_size("gx") // 2, lax.axis_size("gy")
    n = 2 * n_z * n_x
    z, core = gx // 2, gx % 2
    me = gx * n_x + gy

    def partner(k):
        t, u = k // (2 * n_x), (k + 1) % (2 * n_x)
        dz = n_z // 2 + ((t + 1) // 2) * (2 * (t % 2) - 1)
        tz = (z + dz + n_z) % n_z
        tc, tx = (core + u % 2) % 2, (gy + u // 2) % n_x
        return 2 * tz + tc, tx

    barrier = pltpu.get_barrier_semaphore()

    @pl.loop(0, n - 1)
    def _(k):
        px, py = partner(k)
        pl.semaphore_signal(barrier, inc=1, device_id={"gx": px, "gy": py}, device_id_type=MESH)

    lane = lax.broadcasted_iota(jnp.int32, (1, 128), 1)
    row = lax.broadcasted_iota(jnp.int32, (128, 128), 0)
    col = lax.broadcasted_iota(jnp.int32, (128, 128), 1)
    identity = jnp.where(row == col, 1.0, 0.0)
    mats = [identity] * 4
    for e in range(6):
        for w in range(4):
            at = e if w in (0, 3) else 5 - e
            mats[w] = bond_step(mats[w], fields, STARTS[w], order[6 * w + at], lane)
    w0t, w1, w2, w3t = [split(m) for m in mats]
    i0 = lax.broadcasted_iota(jnp.int32, (256, 128), 0)
    g0 = lax.broadcasted_iota(jnp.int32, (256, 128), 1)
    g1 = lax.broadcasted_iota(jnp.int32, (128, 256), 0)
    j1 = lax.broadcasted_iota(jnp.int32, (128, 256), 1)
    left = jnp.where((i0 >> 1) == g0, 1.0, 0.0).astype(jnp.bfloat16)
    right = jnp.where((j1 >> 1) == g1, 1.0, 0.0).astype(jnp.bfloat16)
    ii = lax.broadcasted_iota(jnp.int32, (256, 256), 0)
    jj = lax.broadcasted_iota(jnp.int32, (256, 256), 1)
    same = ((ii ^ jj) & 1) == 0
    w3k = [
        jnp.where(same, dot(dot(left, m).astype(jnp.bfloat16), right), 0.0).astype(jnp.bfloat16)
        for m in w3t
    ]

    for b in range(4):
        rows = slice(128 * b, 128 * (b + 1))
        y = dot_split(split(x_ref[rows, :]), w0t)
        t_ref[rows, :] = dot_split(w1, split(y))
    for n8 in range(2):
        ys = []
        for n7 in range(2):
            t = t_ref[pl.ds(n7 + 2 * n8, 128, stride=4), :]
            ys.append(dot_split(w2, split(t)))
        out = dot_split(split(jnp.concatenate(ys, axis=1)), w3k)
        for n15 in range(2):
            for n7 in range(2):
                send[pl.ds(4 * n8 + 2 * n15 + n7, 64, stride=8), :] = out[
                    64 * n15 : 64 * (n15 + 1), 128 * n7 : 128 * (n7 + 1)
                ]

    pl.semaphore_wait(barrier, n - 1)

    def exchange(source, target, which):
        source, target = source.reshape(n, 4, 128), target.reshape(n, 4, 128)

        @pl.loop(0, n - 1)
        def _(k):
            px, py = partner(k)
            pltpu.make_async_remote_copy(
                src_ref=source.at[px * n_x + py],
                dst_ref=target.at[me],
                send_sem=send_sems.at[which],
                recv_sem=recv_sems.at[which],
                device_id={"gx": px, "gy": py},
                device_id_type=MESH,
            ).start()

        target[me] = source[me]

    def arrived(source, target, which):
        part = pl.ds(0, 4 * (n - 1))
        copy = pltpu.make_async_copy(source.at[part], target.at[part], recv_sems.at[which])
        copy.wait()

    def sent(source, target, which):
        part = pl.ds(0, 4 * (n - 1))
        copy = pltpu.make_async_copy(source.at[part], target.at[part], send_sems.at[which])
        copy.wait()

    exchange(send, held, 0)
    entries = [
        gate_entries(fields[15 + k], fields[16 + k], (1, 128)) for k in range(7)
    ]
    srow = lax.broadcasted_iota(jnp.int32, (8, 128), 0)
    bit1, bit2 = (srow >> 1) & 1, (srow >> 2) & 1
    low, up, down, high, flip = entries[0]
    d15 = jnp.where(bit1 == bit2, jnp.where(bit1 == 0, low, high), jnp.where(bit1 == 0, up, down))
    f15 = jnp.where(bit1 == bit2, 0.0, flip)
    below15 = jnp.where(bit1 == 0, f15, 0.0)
    above15 = jnp.where(bit1 == 0, 0.0, f15)
    low, up, down, high, flip = entries[1]
    d16_0 = jnp.where(bit2 == 0, low, down)
    f16_0 = jnp.where(bit2 == 0, 0.0, flip)
    d16_1 = jnp.where(bit2 == 0, up, high)
    f16_1 = jnp.where(bit2 == 0, flip, 0.0)
    arrived(send, held, 0)

    for c in range(n // 8):
        v = held[32 * c : 32 * (c + 1), :].reshape(4, 8, 128)
        v = v * d15 + pltpu.roll(v, 2, 1) * below15 + pltpu.roll(v, 6, 1) * above15
        v = v.reshape(2, 2, 8, 128)
        v0, v1 = v[:, 0], v[:, 1]
        u0 = v0 * d16_0 + pltpu.roll(v1, 4, 1) * f16_0
        u1 = v1 * d16_1 + pltpu.roll(v0, 4, 1) * f16_1
        v = jnp.stack([u0, u1], axis=1).reshape(32, 128)
        t_ref[32 * c : 32 * (c + 1), :] = mix(v, entries[2], 3)
    total = jnp.zeros((8, 128), jnp.float32)
    for h in range(2):
        v = jnp.concatenate(
            [t_ref[16 * g + 8 * h : 16 * g + 8 * h + 8, :] for g in range(4 * n // 16)], axis=0
        )
        for k in range(4):
            v = mix(v, entries[3 + k], 3 + k)
        total = total + jnp.sum((v * v).reshape(-1, 8, 128), axis=0)
        for g in range(4 * n // 16):
            back[16 * g + 8 * h : 16 * g + 8 * h + 8, :] = v[8 * g : 8 * (g + 1)]

    part_z[...] = jnp.sum(total, axis=0, keepdims=True)

    def small(source, target, slot, px, py, s_sem, r_sem):
        return pltpu.make_async_remote_copy(
            src_ref=source,
            dst_ref=target.at[slot],
            send_sem=s_sem,
            recv_sem=r_sem,
            device_id={"gx": px, "gy": py},
            device_id_type=MESH,
        )

    @pl.loop(1, n_z)
    def _(k):
        tz = (z + k) % n_z
        small(part_z, got_z, z, 2 * tz + core, gy, send_sems.at[2], got_z_sem.at[0]).start()

    got_z[z] = part_z[...]
    exchange(back, final, 1)
    mine = core * n_x + gy
    pltpu.make_async_copy(
        got_z.at[pl.ds(0, n_z - 1)], got_z.at[pl.ds(0, n_z - 1)], got_z_sem.at[0]
    ).wait()
    part_xc[...] = jnp.sum(got_z[...], axis=0)

    @pl.loop(1, 2 * n_x)
    def _(k):
        tc, tx = (core + k % 2) % 2, (gy + k // 2) % n_x
        small(part_xc, got_xc, mine, 2 * z + tc, tx, send_sems.at[3], got_xc_sem.at[0]).start()

    got_xc[mine] = part_xc[...]
    pltpu.make_async_copy(
        got_xc.at[pl.ds(0, 2 * n_x - 1)], got_xc.at[pl.ds(0, 2 * n_x - 1)], got_xc_sem.at[0]
    ).wait()
    summed = jnp.sum(jnp.sum(got_xc[...], axis=0), axis=1, keepdims=True)
    count = float(x_ref.shape[0] * x_ref.shape[1] * n)
    scale = lax.rsqrt(summed / count + EPSILON)
    arrived(back, final, 1)
    for n15 in range(2):
        for n7 in range(2):
            o_ref[pl.ds(n15 * 256 + n7, 128, stride=2), :] = (
                final[pl.ds(2 * n15 + n7, 128, stride=4), :] * scale
            )
    sent(send, held, 0)
    sent(back, final, 1)
    pltpu.make_async_copy(
        got_z.at[pl.ds(0, n_z - 1)], got_z.at[pl.ds(0, n_z - 1)], send_sems.at[2]
    ).wait()
    pltpu.make_async_copy(
        got_xc.at[pl.ds(0, 2 * n_x - 1)], got_xc.at[pl.ds(0, 2 * n_x - 1)], send_sems.at[3]
    ).wait()


def local(initial_state, fields, bond_order):
    amps = initial_state.shape[2]
    n = lax.axis_size("gx") * lax.axis_size("gy")
    n_z, n_xc = lax.axis_size("gx") // 2, 2 * lax.axis_size("gy")
    block = pltpu.VMEM((amps // 128, 128), jnp.float32)
    vmem, smem = pl.BlockSpec(memory_space=pltpu.VMEM), pl.BlockSpec(memory_space=pltpu.SMEM)
    out = pl.pallas_call(
        kernel,
        out_shape=jax.ShapeDtypeStruct((amps // 128, 128), jnp.float32),
        in_specs=[vmem, smem, smem],
        out_specs=vmem,
        scratch_shapes=[
            block,
            block,
            block,
            block,
            block,
            pltpu.VMEM((1, 128), jnp.float32),
            pltpu.VMEM((1, 128), jnp.float32),
            pltpu.VMEM((n_z, 1, 128), jnp.float32),
            pltpu.VMEM((n_xc, 1, 128), jnp.float32),
            pltpu.SemaphoreType.DMA((4,)),
            pltpu.SemaphoreType.DMA((2,)),
            pltpu.SemaphoreType.DMA((1,)),
            pltpu.SemaphoreType.DMA((1,)),
        ],
        compiler_params=pltpu.CompilerParams(collective_id=0, has_side_effects=True),
    )(initial_state.reshape(amps // 128, 128), fields, bond_order.reshape(-1))
    return out.reshape(initial_state.shape)


def solution(mesh):
    placed = (P(("groups", "gx"), "gy", None), P("groups"), P())
    return jax.shard_map(
        local,
        mesh=mesh,
        in_specs=placed,
        out_specs=P(("groups", "gx"), "gy", None),
        check_vma=False,
    )
```

```python
import functools

import jax
import jax.numpy as jnp
from jax import lax
from jax.experimental import pallas as pl
from jax.experimental.pallas import tpu as pltpu
from jax.sharding import PartitionSpec as P

MESH = pl.DeviceIdType.MESH
STEP = 0.15
BOOST = 1.161834242728283
EPSILON = 1e-06
STARTS = (0, 7, 9, 1)


def gate_entries(left, right, shape):
    left = jnp.full(shape, left, jnp.float32)
    right = jnp.full(shape, right, jnp.float32)
    half_sum = 0.5 * (left + right)
    half_diff = 0.5 * (left - right)
    radius = jnp.sqrt(half_diff * half_diff + 4.0)
    grow = jnp.exp(STEP * radius)
    decay = jnp.exp(-STEP * radius)
    cosine = 0.5 * (grow + decay)
    sine_ratio = 0.5 * (grow - decay) / radius
    low = jnp.exp(-STEP * (1.0 + half_sum))
    high = jnp.exp(-STEP * (1.0 - half_sum))
    up = BOOST * (cosine - sine_ratio * half_diff)
    down = BOOST * (cosine + sine_ratio * half_diff)
    flip = -2.0 * BOOST * sine_ratio
    return low, up, down, high, flip


def bond_step(matrix, fields, start, offset, lane):
    low, up, down, high, flip = gate_entries(
        fields[start + offset], fields[start + offset + 1], lane.shape
    )
    first = (lane >> offset) & 1
    second = (lane >> (offset + 1)) & 1
    zero = first == 0
    equal = first == second
    diagonal = jnp.where(equal, jnp.where(zero, low, high), jnp.where(zero, up, down))
    from_below = jnp.where(equal, 0.0, jnp.where(zero, flip, 0.0))
    from_above = jnp.where(equal, 0.0, jnp.where(zero, 0.0, flip))
    shift = jnp.left_shift(1, offset)
    return (
        matrix * diagonal
        + pltpu.roll(matrix, shift, 1) * from_below
        + pltpu.roll(matrix, 128 - shift, 1) * from_above
    )


def split(x):
    high = x.astype(jnp.bfloat16)
    return high, (x - high.astype(jnp.float32)).astype(jnp.bfloat16)


def dot(a, b):
    return jnp.dot(a, b, preferred_element_type=jnp.float32)


def dot_split(a, b):
    return dot(a[0], b[0]) + (dot(a[0], b[1]) + dot(a[1], b[0]))


def mix(value, entries, bit):
    low, up, down, high, flip = entries
    rows = value.shape[0]
    inner = 2**bit
    v = value.reshape(rows // (4 * inner), 2, 2, inner // 8, 8, 128)
    both0, only_first = v[:, 0, 0], v[:, 0, 1]
    only_second, both1 = v[:, 1, 0], v[:, 1, 1]
    new = jnp.stack(
        [
            jnp.stack([low * both0, down * only_first + flip * only_second], axis=1),
            jnp.stack([up * only_second + flip * only_first, high * both1], axis=1),
        ],
        axis=1,
    )
    return new.reshape(value.shape)


def kernel(
    x_hbm,
    fields,
    order,
    o_ref,
    x_ref,
    t_ref,
    send,
    held,
    back,
    final,
    part_z,
    part_xc,
    got_z,
    got_xc,
    send_sems,
    recv_sems,
    got_z_sem,
    got_xc_sem,
    fetch_sem,
    ready,
):
    gx, gy = lax.axis_index("gx"), lax.axis_index("gy")
    n_z, n_x = lax.axis_size("gx") // 2, lax.axis_size("gy")
    plane = 2 * n_x
    n = n_z * plane
    z, core = gx // 2, gx % 2
    mine = core * n_x + gy
    me = z * plane + mine

    fetch = pltpu.make_async_copy(x_hbm, x_ref, fetch_sem)
    fetch.start()

    def at(tz, i):
        return {"gx": 2 * tz + i // n_x, "gy": i % n_x}

    def far_first(t):
        dz = n_z // 2 + ((t + 1) // 2) * (2 * (t % 2) - 1)
        return (z + dz + n_z) % n_z

    barrier = pltpu.get_barrier_semaphore()

    @pl.when(me > 0)
    def _():
        for i in range(plane):

            @pl.when(mine < i)
            def _():
                pl.semaphore_signal(barrier, inc=1, device_id=at(z, i), device_id_type=MESH)

        @pl.loop(z + 1, n_z)
        def _(tz):
            for i in range(plane):
                pl.semaphore_signal(barrier, inc=1, device_id=at(tz, i), device_id_type=MESH)

        pl.semaphore_signal(barrier, inc=1, device_id=at(0, 0), device_id_type=MESH)

    @pl.when(me != 1)
    def _():
        pl.semaphore_wait(barrier, (me + n - 1) % n)

    @pl.when(me > 0)
    def _():
        @pl.loop(0, z)
        def _(tz):
            for i in range(plane):

                def answer():
                    pl.semaphore_signal(
                        ready.at[z], inc=1, device_id=at(tz, i), device_id_type=MESH
                    )

                if i == 0:
                    pl.when(tz > 0)(answer)
                else:
                    answer()

        for i in range(plane):

            @pl.when((i < mine) & (z * plane + i > 0))
            def _():
                pl.semaphore_signal(ready.at[z], inc=1, device_id=at(z, i), device_id_type=MESH)

    @pl.when(me == 0)
    def _():
        @pl.loop(0, n_z)
        def _(tz):
            for i in range(plane):

                def answer():
                    pl.semaphore_signal(
                        ready.at[n_z], inc=1, device_id=at(tz, i), device_id_type=MESH
                    )

                if i == 0:
                    pl.when(tz > 0)(answer)
                else:
                    answer()

    lane = lax.broadcasted_iota(jnp.int32, (1, 128), 1)
    row = lax.broadcasted_iota(jnp.int32, (128, 128), 0)
    col = lax.broadcasted_iota(jnp.int32, (128, 128), 1)
    identity = jnp.where(row == col, 1.0, 0.0)
    mats = [identity] * 4
    for e in range(6):
        for w in range(4):
            step = e if w in (0, 3) else 5 - e
            mats[w] = bond_step(mats[w], fields, STARTS[w], order[w, step], lane)
    w0t, w1, w2, w3t = [split(m) for m in mats]
    i0 = lax.broadcasted_iota(jnp.int32, (256, 128), 0)
    g0 = lax.broadcasted_iota(jnp.int32, (256, 128), 1)
    g1 = lax.broadcasted_iota(jnp.int32, (128, 256), 0)
    j1 = lax.broadcasted_iota(jnp.int32, (128, 256), 1)
    left = jnp.where((i0 >> 1) == g0, 1.0, 0.0).astype(jnp.bfloat16)
    right = jnp.where((j1 >> 1) == g1, 1.0, 0.0).astype(jnp.bfloat16)
    ii = lax.broadcasted_iota(jnp.int32, (256, 256), 0)
    jj = lax.broadcasted_iota(jnp.int32, (256, 256), 1)
    same = ((ii ^ jj) & 1) == 0
    w3k = [
        jnp.where(same, dot(dot(left, m).astype(jnp.bfloat16), right), 0.0).astype(jnp.bfloat16)
        for m in w3t
    ]

    fetch.wait()
    for b in range(4):
        rows = slice(128 * b, 128 * (b + 1))
        y = dot_split(split(x_ref[rows, :]), w0t)
        t_ref[rows, :] = dot_split(w1, split(y))
    for n8 in range(2):
        ys = []
        for n7 in range(2):
            t = t_ref[pl.ds(n7 + 2 * n8, 128, stride=4), :]
            ys.append(dot_split(w2, split(t)))
        out = dot_split(split(jnp.concatenate(ys, axis=1)), w3k)
        for n15 in range(2):
            for n7 in range(2):
                send[pl.ds(4 * n8 + 2 * n15 + n7, 64, stride=8), :] = out[
                    64 * n15 : 64 * (n15 + 1), 128 * n7 : 128 * (n7 + 1)
                ]

    def post(source, target, which, tz, i):
        source, target = source.reshape(n, 4, 128), target.reshape(n, 4, 128)
        pltpu.make_async_remote_copy(
            src_ref=source.at[tz * plane + i],
            dst_ref=target.at[me],
            send_sem=send_sems.at[which],
            recv_sem=recv_sems.at[which],
            device_id=at(tz, i),
            device_id_type=MESH,
        ).start()

    def keep(source, target):
        source, target = source.reshape(n, 4, 128), target.reshape(n, 4, 128)
        target[me] = source[me]

    def post_known(tz):
        for i in range(plane):
            if i == 0:
                pl.when(tz > 0)(functools.partial(post, send, held, 0, tz, i))
            else:
                post(send, held, 0, tz, i)

    def arrived(source, target, which):
        part = pl.ds(0, 4 * (n - 1))
        copy = pltpu.make_async_copy(source.at[part], target.at[part], recv_sems.at[which])
        copy.wait()

    def sent(source, target, which):
        part = pl.ds(0, 4 * (n - 1))
        copy = pltpu.make_async_copy(source.at[part], target.at[part], send_sems.at[which])
        copy.wait()

    @pl.loop(0, n_z - 1)
    def _(t):
        tz = far_first(t)

        @pl.when((tz < z) | (me == 0))
        def _():
            post_known(tz)

    @pl.when((me > 0) & (mine < plane - 1))
    def _():
        pl.semaphore_wait(ready.at[z], plane - 1 - mine)

    for i in range(plane):

        @pl.when((i != mine) & (z * plane + i > 0))
        def _():
            post(send, held, 0, z, i)

    @pl.when(me > 0)
    def _():
        @pl.loop(z + 1, n_z)
        def _(tz):
            pl.semaphore_wait(ready.at[tz], plane)
            post_known(tz)

        pl.semaphore_wait(ready.at[n_z], 1)
        post(send, held, 0, 0, 0)

    keep(send, held)
    entries = [
        gate_entries(fields[15 + k], fields[16 + k], (1, 128)) for k in range(7)
    ]
    srow = lax.broadcasted_iota(jnp.int32, (8, 128), 0)
    bit1, bit2 = (srow >> 1) & 1, (srow >> 2) & 1
    low, up, down, high, flip = entries[0]
    d15 = jnp.where(bit1 == bit2, jnp.where(bit1 == 0, low, high), jnp.where(bit1 == 0, up, down))
    f15 = jnp.where(bit1 == bit2, 0.0, flip)
    below15 = jnp.where(bit1 == 0, f15, 0.0)
    above15 = jnp.where(bit1 == 0, 0.0, f15)
    low, up, down, high, flip = entries[1]
    d16_0 = jnp.where(bit2 == 0, low, down)
    f16_0 = jnp.where(bit2 == 0, 0.0, flip)
    d16_1 = jnp.where(bit2 == 0, up, high)
    f16_1 = jnp.where(bit2 == 0, flip, 0.0)
    arrived(send, held, 0)

    for c in range(n // 8):
        v = held[32 * c : 32 * (c + 1), :].reshape(4, 8, 128)
        v = v * d15 + pltpu.roll(v, 2, 1) * below15 + pltpu.roll(v, 6, 1) * above15
        v = v.reshape(2, 2, 8, 128)
        v0, v1 = v[:, 0], v[:, 1]
        u0 = v0 * d16_0 + pltpu.roll(v1, 4, 1) * f16_0
        u1 = v1 * d16_1 + pltpu.roll(v0, 4, 1) * f16_1
        v = jnp.stack([u0, u1], axis=1).reshape(32, 128)
        t_ref[32 * c : 32 * (c + 1), :] = mix(v, entries[2], 3)
    total = jnp.zeros((8, 128), jnp.float32)
    for h in range(2):
        v = jnp.concatenate(
            [t_ref[16 * g + 8 * h : 16 * g + 8 * h + 8, :] for g in range(4 * n // 16)], axis=0
        )
        for k in range(4):
            v = mix(v, entries[3 + k], 3 + k)
        total = total + jnp.sum((v * v).reshape(-1, 8, 128), axis=0)
        for g in range(4 * n // 16):
            back[16 * g + 8 * h : 16 * g + 8 * h + 8, :] = v[8 * g : 8 * (g + 1)]

    part_z[...] = jnp.sum(total, axis=0, keepdims=True)

    def small(source, target, slot, px, py, s_sem, r_sem):
        return pltpu.make_async_remote_copy(
            src_ref=source,
            dst_ref=target.at[slot],
            send_sem=s_sem,
            recv_sem=r_sem,
            device_id={"gx": px, "gy": py},
            device_id_type=MESH,
        )

    @pl.loop(1, n_z)
    def _(k):
        tz = (z + k) % n_z
        small(part_z, got_z, z, 2 * tz + core, gy, send_sems.at[2], got_z_sem.at[0]).start()

    got_z[z] = part_z[...]

    @pl.loop(0, n_z - 1)
    def _(t):
        tz = far_first(t)
        for i in range(plane):
            post(back, final, 1, tz, i)

    for i in range(plane):

        @pl.when(i != mine)
        def _():
            post(back, final, 1, z, i)

    keep(back, final)
    pltpu.make_async_copy(
        got_z.at[pl.ds(0, n_z - 1)], got_z.at[pl.ds(0, n_z - 1)], got_z_sem.at[0]
    ).wait()
    part_xc[...] = jnp.sum(got_z[...], axis=0)

    @pl.loop(1, 2 * n_x)
    def _(k):
        tc, tx = (core + k % 2) % 2, (gy + k // 2) % n_x
        small(part_xc, got_xc, mine, 2 * z + tc, tx, send_sems.at[3], got_xc_sem.at[0]).start()

    got_xc[mine] = part_xc[...]
    pltpu.make_async_copy(
        got_xc.at[pl.ds(0, 2 * n_x - 1)], got_xc.at[pl.ds(0, 2 * n_x - 1)], got_xc_sem.at[0]
    ).wait()
    summed = jnp.sum(jnp.sum(got_xc[...], axis=0), axis=1, keepdims=True)
    count = float(x_ref.shape[0] * x_ref.shape[1] * n)
    scale = lax.rsqrt(summed / count + EPSILON)
    arrived(back, final, 1)
    for n15 in range(2):
        for n7 in range(2):
            o_ref[pl.ds(n15 * 256 + n7, 128, stride=2), :] = (
                final[pl.ds(2 * n15 + n7, 128, stride=4), :] * scale
            )
    sent(send, held, 0)
    sent(back, final, 1)
    pltpu.make_async_copy(
        got_z.at[pl.ds(0, n_z - 1)], got_z.at[pl.ds(0, n_z - 1)], send_sems.at[2]
    ).wait()
    pltpu.make_async_copy(
        got_xc.at[pl.ds(0, 2 * n_x - 1)], got_xc.at[pl.ds(0, 2 * n_x - 1)], send_sems.at[3]
    ).wait()


def local(initial_state, fields, bond_order):
    amps = initial_state.shape[2]
    n = lax.axis_size("gx") * lax.axis_size("gy")
    n_z, n_xc = lax.axis_size("gx") // 2, 2 * lax.axis_size("gy")
    block = pltpu.VMEM((amps // 128, 128), jnp.float32)
    vmem, smem = pl.BlockSpec(memory_space=pltpu.VMEM), pl.BlockSpec(memory_space=pltpu.SMEM)
    out = pl.pallas_call(
        kernel,
        out_shape=jax.ShapeDtypeStruct((amps // 128, 128), jnp.float32),
        in_specs=[pl.BlockSpec(memory_space=pl.ANY), smem, smem],
        out_specs=vmem,
        scratch_shapes=[
            block,
            block,
            block,
            block,
            block,
            block,
            pltpu.VMEM((1, 128), jnp.float32),
            pltpu.VMEM((1, 128), jnp.float32),
            pltpu.VMEM((n_z, 1, 128), jnp.float32),
            pltpu.VMEM((n_xc, 1, 128), jnp.float32),
            pltpu.SemaphoreType.DMA((4,)),
            pltpu.SemaphoreType.DMA((2,)),
            pltpu.SemaphoreType.DMA((1,)),
            pltpu.SemaphoreType.DMA((1,)),
            pltpu.SemaphoreType.DMA,
            pltpu.SemaphoreType.REGULAR((n_z + 1,)),
        ],
        compiler_params=pltpu.CompilerParams(collective_id=0, has_side_effects=True),
    )(initial_state.reshape(amps // 128, 128), fields, bond_order)
    return out.reshape(initial_state.shape)


def solution(mesh):
    placed = (P(("groups", "gx"), "gy", None), P("groups"), P())
    return jax.shard_map(
        local,
        mesh=mesh,
        in_specs=placed,
        out_specs=P(("groups", "gx"), "gy", None),
        check_vma=False,
    )
```

```python
import functools

import jax
import jax.numpy as jnp
from jax import lax
from jax.experimental import pallas as pl
from jax.experimental.pallas import tpu as pltpu
from jax.sharding import PartitionSpec as P

MESH = pl.DeviceIdType.MESH
STEP = 0.15
BOOST = 1.161834242728283
EPSILON = 1e-06
STARTS = (0, 7, 9, 1)


def gate_entries(left, right, shape):
    left = jnp.full(shape, left, jnp.float32)
    right = jnp.full(shape, right, jnp.float32)
    half_sum = 0.5 * (left + right)
    half_diff = 0.5 * (left - right)
    radius = jnp.sqrt(half_diff * half_diff + 4.0)
    grow = jnp.exp(STEP * radius)
    decay = jnp.exp(-STEP * radius)
    cosine = 0.5 * (grow + decay)
    sine_ratio = 0.5 * (grow - decay) / radius
    low = jnp.exp(-STEP * (1.0 + half_sum))
    high = jnp.exp(-STEP * (1.0 - half_sum))
    up = BOOST * (cosine - sine_ratio * half_diff)
    down = BOOST * (cosine + sine_ratio * half_diff)
    flip = -2.0 * BOOST * sine_ratio
    return low, up, down, high, flip


def bond_step(matrix, fields, start, offset, lane):
    low, up, down, high, flip = gate_entries(
        fields[start + offset], fields[start + offset + 1], lane.shape
    )
    first = (lane >> offset) & 1
    second = (lane >> (offset + 1)) & 1
    zero = first == 0
    equal = first == second
    diagonal = jnp.where(equal, jnp.where(zero, low, high), jnp.where(zero, up, down))
    from_below = jnp.where(equal, 0.0, jnp.where(zero, flip, 0.0))
    from_above = jnp.where(equal, 0.0, jnp.where(zero, 0.0, flip))
    shift = jnp.left_shift(1, offset)
    return (
        matrix * diagonal
        + pltpu.roll(matrix, shift, 1) * from_below
        + pltpu.roll(matrix, 128 - shift, 1) * from_above
    )


def split(x):
    high = x.astype(jnp.bfloat16)
    return high, (x - high.astype(jnp.float32)).astype(jnp.bfloat16)


def dot(a, b):
    return jnp.dot(a, b, preferred_element_type=jnp.float32)


def dot_split(a, b):
    return dot(a[0], b[0]) + (dot(a[0], b[1]) + dot(a[1], b[0]))


def mix(value, entries, bit):
    low, up, down, high, flip = entries
    rows = value.shape[0]
    inner = 2**bit
    v = value.reshape(rows // (4 * inner), 2, 2, inner // 8, 8, 128)
    both0, only_first = v[:, 0, 0], v[:, 0, 1]
    only_second, both1 = v[:, 1, 0], v[:, 1, 1]
    new = jnp.stack(
        [
            jnp.stack([low * both0, down * only_first + flip * only_second], axis=1),
            jnp.stack([up * only_second + flip * only_first, high * both1], axis=1),
        ],
        axis=1,
    )
    return new.reshape(value.shape)


def kernel(
    x_hbm,
    fields_hbm,
    order_hbm,
    o_ref,
    fields,
    order,
    x_ref,
    t_ref,
    send,
    held,
    back,
    final,
    part_z,
    part_xc,
    got_z,
    got_xc,
    send_sems,
    recv_sems,
    got_z_sem,
    got_xc_sem,
    fetch_sems,
    ready,
):
    gx, gy = lax.axis_index("gx"), lax.axis_index("gy")
    n_z, n_x = lax.axis_size("gx") // 2, lax.axis_size("gy")
    plane = 2 * n_x
    n = n_z * plane
    z, core = gx // 2, gx % 2
    mine = core * n_x + gy
    me = z * plane + mine

    fetch = pltpu.make_async_copy(x_hbm, x_ref, fetch_sems.at[0])
    fetch_fields = pltpu.make_async_copy(fields_hbm, fields, fetch_sems.at[1])
    fetch_order = pltpu.make_async_copy(order_hbm, order, fetch_sems.at[2])
    fetch_fields.start()
    fetch_order.start()
    fetch.start()

    def at(tz, i):
        return {"gx": 2 * tz + i // n_x, "gy": i % n_x}

    def far_first(t):
        dz = n_z // 2 + ((t + 1) // 2) * (2 * (t % 2) - 1)
        return (z + dz + n_z) % n_z

    barrier = pltpu.get_barrier_semaphore()

    def greet(device):
        pl.semaphore_signal(barrier, inc=1, device_id=device, device_id_type=MESH)

    @pl.when(me > 0)
    def _():
        for i in range(plane):

            @pl.when((mine != i) & (z * plane + i > 0))
            def _():
                greet(at(z, i))

    lane = lax.broadcasted_iota(jnp.int32, (1, 128), 1)
    row = lax.broadcasted_iota(jnp.int32, (128, 128), 0)
    col = lax.broadcasted_iota(jnp.int32, (128, 128), 1)
    fetch_fields.wait()
    fetch_order.wait()
    identity = jnp.where(row == col, 1.0, 0.0)
    mats = [identity] * 4
    for e in range(6):
        for w in range(4):
            step = e if w in (0, 3) else 5 - e
            mats[w] = bond_step(mats[w], fields, STARTS[w], order[w, step], lane)
    w0t, w1, w2, w3t = [split(m) for m in mats]
    i0 = lax.broadcasted_iota(jnp.int32, (256, 128), 0)
    g0 = lax.broadcasted_iota(jnp.int32, (256, 128), 1)
    g1 = lax.broadcasted_iota(jnp.int32, (128, 256), 0)
    j1 = lax.broadcasted_iota(jnp.int32, (128, 256), 1)
    left = jnp.where((i0 >> 1) == g0, 1.0, 0.0).astype(jnp.bfloat16)
    right = jnp.where((j1 >> 1) == g1, 1.0, 0.0).astype(jnp.bfloat16)
    ii = lax.broadcasted_iota(jnp.int32, (256, 256), 0)
    jj = lax.broadcasted_iota(jnp.int32, (256, 256), 1)
    same = ((ii ^ jj) & 1) == 0
    w3k = [
        jnp.where(same, dot(dot(left, m).astype(jnp.bfloat16), right), 0.0).astype(jnp.bfloat16)
        for m in w3t
    ]

    @pl.when(me > 0)
    def _():
        whole = jnp.where(z > 0, plane - 1, plane - 2)
        pl.semaphore_wait(barrier, whole + z)

        @pl.loop(0, z)
        def _(tz):
            @pl.when(tz * plane + mine > 0)
            def _():
                pl.semaphore_signal(
                    ready.at[z], inc=1, device_id=at(tz, mine), device_id_type=MESH
                )

        @pl.loop(z + 1, n_z)
        def _(tz):
            greet(at(tz, mine))

        @pl.when(mine == 1)
        def _():
            greet(at(0, 0))

            @pl.when(z == 0)
            def _():
                @pl.loop(1, n_z)
                def _(tz):
                    greet(at(tz, 0))

    fetch.wait()
    for b in range(4):
        rows = slice(128 * b, 128 * (b + 1))
        y = dot_split(split(x_ref[rows, :]), w0t)
        t_ref[rows, :] = dot_split(w1, split(y))
    for n8 in range(2):
        ys = []
        for n7 in range(2):
            t = t_ref[pl.ds(n7 + 2 * n8, 128, stride=4), :]
            ys.append(dot_split(w2, split(t)))
        out = dot_split(split(jnp.concatenate(ys, axis=1)), w3k)
        for n15 in range(2):
            for n7 in range(2):
                send[pl.ds(4 * n8 + 2 * n15 + n7, 64, stride=8), :] = out[
                    64 * n15 : 64 * (n15 + 1), 128 * n7 : 128 * (n7 + 1)
                ]

    def post(source, target, which, tz, i):
        source, target = source.reshape(n, 4, 128), target.reshape(n, 4, 128)
        pltpu.make_async_remote_copy(
            src_ref=source.at[tz * plane + i],
            dst_ref=target.at[me],
            send_sem=send_sems.at[which],
            recv_sem=recv_sems.at[which],
            device_id=at(tz, i),
            device_id_type=MESH,
        ).start()

    def keep(source, target):
        source, target = source.reshape(n, 4, 128), target.reshape(n, 4, 128)
        target[me] = source[me]

    def post_known(tz):
        for i in range(plane):
            if i == 0:
                pl.when(tz > 0)(functools.partial(post, send, held, 0, tz, i))
            else:
                post(send, held, 0, tz, i)

    def arrived(source, target, which):
        part = pl.ds(0, 4 * (n - 1))
        copy = pltpu.make_async_copy(source.at[part], target.at[part], recv_sems.at[which])
        copy.wait()

    def sent(source, target, which):
        part = pl.ds(0, 4 * (n - 1))
        copy = pltpu.make_async_copy(source.at[part], target.at[part], send_sems.at[which])
        copy.wait()

    @pl.when(me == 0)
    def _():
        pl.semaphore_wait(barrier, n_z)

        @pl.loop(0, n_z)
        def _(t):
            tz = far_first(t)
            for i in range(plane):

                @pl.when(tz * plane + i > 0)
                def _():
                    pl.semaphore_signal(
                        ready.at[n_z], inc=1, device_id=at(tz, i), device_id_type=MESH
                    )

    @pl.loop(0, n_z - 1)
    def _(t):
        tz = far_first(t)

        @pl.when((tz < z) | (me == 0))
        def _():
            post_known(tz)

    for i in range(plane):

        @pl.when((i != mine) & (z * plane + i > 0))
        def _():
            post(send, held, 0, z, i)

    @pl.when(me > 0)
    def _():
        @pl.loop(z + 1, n_z)
        def _(tz):
            pl.semaphore_wait(ready.at[tz], 1)
            post_known(tz)

        pl.semaphore_wait(ready.at[n_z], 1)
        post(send, held, 0, 0, 0)

    keep(send, held)
    entries = [
        gate_entries(fields[15 + k], fields[16 + k], (1, 128)) for k in range(7)
    ]
    srow = lax.broadcasted_iota(jnp.int32, (8, 128), 0)
    bit1, bit2 = (srow >> 1) & 1, (srow >> 2) & 1
    low, up, down, high, flip = entries[0]
    d15 = jnp.where(bit1 == bit2, jnp.where(bit1 == 0, low, high), jnp.where(bit1 == 0, up, down))
    f15 = jnp.where(bit1 == bit2, 0.0, flip)
    below15 = jnp.where(bit1 == 0, f15, 0.0)
    above15 = jnp.where(bit1 == 0, 0.0, f15)
    low, up, down, high, flip = entries[1]
    d16_0 = jnp.where(bit2 == 0, low, down)
    f16_0 = jnp.where(bit2 == 0, 0.0, flip)
    d16_1 = jnp.where(bit2 == 0, up, high)
    f16_1 = jnp.where(bit2 == 0, flip, 0.0)
    arrived(send, held, 0)

    for c in range(n // 8):
        v = held[32 * c : 32 * (c + 1), :].reshape(4, 8, 128)
        v = v * d15 + pltpu.roll(v, 2, 1) * below15 + pltpu.roll(v, 6, 1) * above15
        v = v.reshape(2, 2, 8, 128)
        v0, v1 = v[:, 0], v[:, 1]
        u0 = v0 * d16_0 + pltpu.roll(v1, 4, 1) * f16_0
        u1 = v1 * d16_1 + pltpu.roll(v0, 4, 1) * f16_1
        v = jnp.stack([u0, u1], axis=1).reshape(32, 128)
        t_ref[32 * c : 32 * (c + 1), :] = mix(v, entries[2], 3)
    total = jnp.zeros((8, 128), jnp.float32)
    for h in range(2):
        v = jnp.concatenate(
            [t_ref[16 * g + 8 * h : 16 * g + 8 * h + 8, :] for g in range(4 * n // 16)], axis=0
        )
        for k in range(4):
            v = mix(v, entries[3 + k], 3 + k)
        total = total + jnp.sum((v * v).reshape(-1, 8, 128), axis=0)
        for g in range(4 * n // 16):
            back[16 * g + 8 * h : 16 * g + 8 * h + 8, :] = v[8 * g : 8 * (g + 1)]

    part_z[...] = jnp.sum(total, axis=0, keepdims=True)

    def small(source, target, slot, px, py, s_sem, r_sem):
        return pltpu.make_async_remote_copy(
            src_ref=source,
            dst_ref=target.at[slot],
            send_sem=s_sem,
            recv_sem=r_sem,
            device_id={"gx": px, "gy": py},
            device_id_type=MESH,
        )

    @pl.loop(1, n_z)
    def _(k):
        tz = (z + k) % n_z
        small(part_z, got_z, z, 2 * tz + core, gy, send_sems.at[2], got_z_sem.at[0]).start()

    got_z[z] = part_z[...]

    @pl.loop(0, n_z - 1)
    def _(t):
        tz = far_first(t)
        for i in range(plane):
            post(back, final, 1, tz, i)

    for i in range(plane):

        @pl.when(i != mine)
        def _():
            post(back, final, 1, z, i)

    keep(back, final)
    pltpu.make_async_copy(
        got_z.at[pl.ds(0, n_z - 1)], got_z.at[pl.ds(0, n_z - 1)], got_z_sem.at[0]
    ).wait()
    part_xc[...] = jnp.sum(got_z[...], axis=0)

    @pl.loop(1, 2 * n_x)
    def _(k):
        tc, tx = (core + k % 2) % 2, (gy + k // 2) % n_x
        small(part_xc, got_xc, mine, 2 * z + tc, tx, send_sems.at[3], got_xc_sem.at[0]).start()

    got_xc[mine] = part_xc[...]
    pltpu.make_async_copy(
        got_xc.at[pl.ds(0, 2 * n_x - 1)], got_xc.at[pl.ds(0, 2 * n_x - 1)], got_xc_sem.at[0]
    ).wait()
    summed = jnp.sum(jnp.sum(got_xc[...], axis=0), axis=1, keepdims=True)
    count = float(x_ref.shape[0] * x_ref.shape[1] * n)
    scale = lax.rsqrt(summed / count + EPSILON)
    arrived(back, final, 1)
    for n15 in range(2):
        for n7 in range(2):
            o_ref[pl.ds(n15 * 256 + n7, 128, stride=2), :] = (
                final[pl.ds(2 * n15 + n7, 128, stride=4), :] * scale
            )
    sent(send, held, 0)
    sent(back, final, 1)
    pltpu.make_async_copy(
        got_z.at[pl.ds(0, n_z - 1)], got_z.at[pl.ds(0, n_z - 1)], send_sems.at[2]
    ).wait()
    pltpu.make_async_copy(
        got_xc.at[pl.ds(0, 2 * n_x - 1)], got_xc.at[pl.ds(0, 2 * n_x - 1)], send_sems.at[3]
    ).wait()


def local(initial_state, fields, bond_order):
    amps = initial_state.shape[2]
    n = lax.axis_size("gx") * lax.axis_size("gy")
    n_z, n_xc = lax.axis_size("gx") // 2, 2 * lax.axis_size("gy")
    block = pltpu.VMEM((amps // 128, 128), jnp.float32)
    vmem, hbm = pl.BlockSpec(memory_space=pltpu.VMEM), pl.BlockSpec(memory_space=pltpu.HBM)
    pin = functools.partial(pltpu.with_memory_space_constraint, memory_space=pltpu.HBM)
    out = pl.pallas_call(
        kernel,
        out_shape=jax.ShapeDtypeStruct((amps // 128, 128), jnp.float32),
        in_specs=[hbm, hbm, hbm],
        out_specs=vmem,
        scratch_shapes=[
            pltpu.SMEM(fields.shape, jnp.float32),
            pltpu.SMEM(bond_order.shape, jnp.int32),
            block,
            block,
            block,
            block,
            block,
            block,
            pltpu.VMEM((1, 128), jnp.float32),
            pltpu.VMEM((1, 128), jnp.float32),
            pltpu.VMEM((n_z, 1, 128), jnp.float32),
            pltpu.VMEM((n_xc, 1, 128), jnp.float32),
            pltpu.SemaphoreType.DMA((4,)),
            pltpu.SemaphoreType.DMA((2,)),
            pltpu.SemaphoreType.DMA((1,)),
            pltpu.SemaphoreType.DMA((1,)),
            pltpu.SemaphoreType.DMA((3,)),
            pltpu.SemaphoreType.REGULAR((n_z + 1,)),
        ],
        compiler_params=pltpu.CompilerParams(
            collective_id=0, has_side_effects=True, vmem_limit_bytes=4 * 2**20
        ),
    )(
        pin(initial_state.reshape(amps // 128, 128)), pin(fields), pin(bond_order)
    )
    return out.reshape(initial_state.shape)


def solution(mesh):
    placed = (P(("groups", "gx"), "gy", None), P("groups"), P())
    return jax.shard_map(
        local,
        mesh=mesh,
        in_specs=placed,
        out_specs=P(("groups", "gx"), "gy", None),
        check_vma=False,
    )
```

```python
import functools

import jax
import jax.numpy as jnp
from jax import lax
from jax.experimental import pallas as pl
from jax.experimental.pallas import tpu as pltpu
from jax.sharding import PartitionSpec as P

MESH = pl.DeviceIdType.MESH
STEP = 0.15
BOOST = 1.161834242728283
EPSILON = 1e-06
STARTS = (0, 7, 9, 1)


def gate_entries(left, right, shape):
    left = jnp.full(shape, left, jnp.float32)
    right = jnp.full(shape, right, jnp.float32)
    half_sum = 0.5 * (left + right)
    half_diff = 0.5 * (left - right)
    radius = jnp.sqrt(half_diff * half_diff + 4.0)
    grow = jnp.exp(STEP * radius)
    decay = jnp.exp(-STEP * radius)
    cosine = 0.5 * (grow + decay)
    sine_ratio = 0.5 * (grow - decay) / radius
    low = jnp.exp(-STEP * (1.0 + half_sum))
    high = jnp.exp(-STEP * (1.0 - half_sum))
    up = BOOST * (cosine - sine_ratio * half_diff)
    down = BOOST * (cosine + sine_ratio * half_diff)
    flip = -2.0 * BOOST * sine_ratio
    return low, up, down, high, flip


def bond_step(matrix, fields, start, offset, lane):
    low, up, down, high, flip = gate_entries(
        fields[start + offset], fields[start + offset + 1], lane.shape
    )
    first = (lane >> offset) & 1
    second = (lane >> (offset + 1)) & 1
    zero = first == 0
    equal = first == second
    diagonal = jnp.where(equal, jnp.where(zero, low, high), jnp.where(zero, up, down))
    from_below = jnp.where(equal, 0.0, jnp.where(zero, flip, 0.0))
    from_above = jnp.where(equal, 0.0, jnp.where(zero, 0.0, flip))
    shift = jnp.left_shift(1, offset)
    return (
        matrix * diagonal
        + pltpu.roll(matrix, shift, 1) * from_below
        + pltpu.roll(matrix, 128 - shift, 1) * from_above
    )


def split(x):
    high = x.astype(jnp.bfloat16)
    return high, (x - high.astype(jnp.float32)).astype(jnp.bfloat16)


def dot(a, b):
    return jnp.dot(a, b, preferred_element_type=jnp.float32)


def dot_split(a, b):
    return dot(a[0], b[0]) + (dot(a[0], b[1]) + dot(a[1], b[0]))


def mix(value, entries, bit):
    low, up, down, high, flip = entries
    rows = value.shape[0]
    inner = 2**bit
    v = value.reshape(rows // (4 * inner), 2, 2, inner // 8, 8, 128)
    both0, only_first = v[:, 0, 0], v[:, 0, 1]
    only_second, both1 = v[:, 1, 0], v[:, 1, 1]
    new = jnp.stack(
        [
            jnp.stack([low * both0, down * only_first + flip * only_second], axis=1),
            jnp.stack([up * only_second + flip * only_first, high * both1], axis=1),
        ],
        axis=1,
    )
    return new.reshape(value.shape)


def kernel(
    x_hbm,
    fields_hbm,
    order_hbm,
    o_ref,
    fields,
    order,
    x_ref,
    t_ref,
    send,
    held,
    back,
    final,
    part_z,
    part_xc,
    got_z,
    got_xc,
    send_sems,
    recv_sems,
    got_z_sem,
    got_xc_sem,
    fetch_sems,
    ready,
):
    gx, gy = lax.axis_index("gx"), lax.axis_index("gy")
    n_z, n_x = lax.axis_size("gx") // 2, lax.axis_size("gy")
    plane = 2 * n_x
    n = n_z * plane
    z, core = gx // 2, gx % 2
    mine = core * n_x + gy
    me = z * plane + mine

    fetch = pltpu.make_async_copy(x_hbm, x_ref, fetch_sems.at[0])
    fetch_fields = pltpu.make_async_copy(fields_hbm, fields, fetch_sems.at[1])
    fetch_order = pltpu.make_async_copy(order_hbm, order, fetch_sems.at[2])
    fetch_fields.start()
    fetch_order.start()
    fetch.start()

    def at(tz, i):
        return {"gx": 2 * tz + i // n_x, "gy": i % n_x}

    def far_first(t):
        dz = n_z // 2 + ((t + 1) // 2) * (2 * (t % 2) - 1)
        return (z + dz + n_z) % n_z

    barrier = pltpu.get_barrier_semaphore()

    def greet(device):
        pl.semaphore_signal(barrier, inc=1, device_id=device, device_id_type=MESH)

    @pl.when(me > 0)
    def _():
        for i in range(plane):

            @pl.when((mine != i) & (z * plane + i > 0))
            def _():
                greet(at(z, i))

        @pl.loop(z + 1, n_z)
        def _(tz):
            greet(at(tz, mine))

        greet(at(0, 0))

    lane = lax.broadcasted_iota(jnp.int32, (1, 128), 1)
    row = lax.broadcasted_iota(jnp.int32, (128, 128), 0)
    col = lax.broadcasted_iota(jnp.int32, (128, 128), 1)
    fetch_fields.wait()
    fetch_order.wait()
    identity = jnp.where(row == col, 1.0, 0.0)
    mats = [identity] * 4
    for e in range(6):
        for w in range(4):
            step = e if w in (0, 3) else 5 - e
            mats[w] = bond_step(mats[w], fields, STARTS[w], order[w, step], lane)
    w0t, w1, w2, w3t = [split(m) for m in mats]
    i0 = lax.broadcasted_iota(jnp.int32, (256, 128), 0)
    g0 = lax.broadcasted_iota(jnp.int32, (256, 128), 1)
    g1 = lax.broadcasted_iota(jnp.int32, (128, 256), 0)
    j1 = lax.broadcasted_iota(jnp.int32, (128, 256), 1)
    left = jnp.where((i0 >> 1) == g0, 1.0, 0.0).astype(jnp.bfloat16)
    right = jnp.where((j1 >> 1) == g1, 1.0, 0.0).astype(jnp.bfloat16)
    ii = lax.broadcasted_iota(jnp.int32, (256, 256), 0)
    jj = lax.broadcasted_iota(jnp.int32, (256, 256), 1)
    same = ((ii ^ jj) & 1) == 0
    w3k = [
        jnp.where(same, dot(dot(left, m).astype(jnp.bfloat16), right), 0.0).astype(jnp.bfloat16)
        for m in w3t
    ]

    @pl.when(me > 0)
    def _():
        whole = jnp.where(z > 0, plane - 1, plane - 2)
        column = jnp.where((z > 0) & (mine == 0), z - 1, z)
        pl.semaphore_wait(barrier, whole + column)

        @pl.loop(0, n_z - 1)
        def _(t):
            tz = far_first(t)

            @pl.when((tz < z) & (tz * plane + mine > 0))
            def _():
                pl.semaphore_signal(
                    ready.at[z], inc=1, device_id=at(tz, mine), device_id_type=MESH
                )

    @pl.when(z > 0)
    def _():
        for i in range(plane):

            @pl.when(mine != i)
            def _():
                pl.semaphore_signal(
                    ready.at[n_z + 1], inc=1, device_id=at(z, i), device_id_type=MESH
                )

    @pl.when(me == 0)
    def _():
        pl.semaphore_wait(barrier, n - 1)

        @pl.loop(0, n_z)
        def _(t):
            tz = far_first(t)
            for i in range(plane):

                @pl.when(tz * plane + i > 0)
                def _():
                    pl.semaphore_signal(
                        ready.at[n_z], inc=1, device_id=at(tz, i), device_id_type=MESH
                    )

    fetch.wait()
    for b in range(4):
        rows = slice(128 * b, 128 * (b + 1))
        y = dot_split(split(x_ref[rows, :]), w0t)
        t_ref[rows, :] = dot_split(w1, split(y))
    for n8 in range(2):
        ys = []
        for n7 in range(2):
            t = t_ref[pl.ds(n7 + 2 * n8, 128, stride=4), :]
            ys.append(dot_split(w2, split(t)))
        out = dot_split(split(jnp.concatenate(ys, axis=1)), w3k)
        for n15 in range(2):
            for n7 in range(2):
                send[pl.ds(4 * n8 + 2 * n15 + n7, 64, stride=8), :] = out[
                    64 * n15 : 64 * (n15 + 1), 128 * n7 : 128 * (n7 + 1)
                ]

    def post(source, target, which, tz, i):
        source, target = source.reshape(n, 4, 128), target.reshape(n, 4, 128)
        pltpu.make_async_remote_copy(
            src_ref=source.at[tz * plane + i],
            dst_ref=target.at[me],
            send_sem=send_sems.at[which],
            recv_sem=recv_sems.at[which],
            device_id=at(tz, i),
            device_id_type=MESH,
        ).start()

    def keep(source, target):
        source, target = source.reshape(n, 4, 128), target.reshape(n, 4, 128)
        target[me] = source[me]

    def post_known(tz):
        for i in range(plane):
            if i == 0:
                pl.when(tz > 0)(functools.partial(post, send, held, 0, tz, i))
            else:
                post(send, held, 0, tz, i)

    def arrived(source, target, which):
        part = pl.ds(0, 4 * (n - 1))
        copy = pltpu.make_async_copy(source.at[part], target.at[part], recv_sems.at[which])
        copy.wait()

    def sent(source, target, which):
        part = pl.ds(0, 4 * (n - 1))
        copy = pltpu.make_async_copy(source.at[part], target.at[part], send_sems.at[which])
        copy.wait()

    @pl.when(z > 0)
    def _():
        pl.semaphore_wait(ready.at[n_z + 1], plane - 1)

    @pl.loop(0, n_z - 1)
    def _(t):
        tz = far_first(t)

        @pl.when((tz < z) | (me == 0))
        def _():
            post_known(tz)

    for i in range(plane):

        @pl.when((i != mine) & (z * plane + i > 0))
        def _():
            post(send, held, 0, z, i)

    @pl.when(me > 0)
    def _():
        @pl.loop(z + 1, n_z)
        def _(tz):
            pl.semaphore_wait(ready.at[tz], 1)
            post_known(tz)

        pl.semaphore_wait(ready.at[n_z], 1)
        post(send, held, 0, 0, 0)

    keep(send, held)
    entries = [
        gate_entries(fields[15 + k], fields[16 + k], (1, 128)) for k in range(7)
    ]
    srow = lax.broadcasted_iota(jnp.int32, (8, 128), 0)
    bit1, bit2 = (srow >> 1) & 1, (srow >> 2) & 1
    low, up, down, high, flip = entries[0]
    d15 = jnp.where(bit1 == bit2, jnp.where(bit1 == 0, low, high), jnp.where(bit1 == 0, up, down))
    f15 = jnp.where(bit1 == bit2, 0.0, flip)
    below15 = jnp.where(bit1 == 0, f15, 0.0)
    above15 = jnp.where(bit1 == 0, 0.0, f15)
    low, up, down, high, flip = entries[1]
    d16_0 = jnp.where(bit2 == 0, low, down)
    f16_0 = jnp.where(bit2 == 0, 0.0, flip)
    d16_1 = jnp.where(bit2 == 0, up, high)
    f16_1 = jnp.where(bit2 == 0, flip, 0.0)
    arrived(send, held, 0)

    for c in range(n // 8):
        v = held[32 * c : 32 * (c + 1), :].reshape(4, 8, 128)
        v = v * d15 + pltpu.roll(v, 2, 1) * below15 + pltpu.roll(v, 6, 1) * above15
        v = v.reshape(2, 2, 8, 128)
        v0, v1 = v[:, 0], v[:, 1]
        u0 = v0 * d16_0 + pltpu.roll(v1, 4, 1) * f16_0
        u1 = v1 * d16_1 + pltpu.roll(v0, 4, 1) * f16_1
        v = jnp.stack([u0, u1], axis=1).reshape(32, 128)
        t_ref[32 * c : 32 * (c + 1), :] = mix(v, entries[2], 3)
    total = jnp.zeros((8, 128), jnp.float32)
    for h in range(2):
        v = jnp.concatenate(
            [t_ref[16 * g + 8 * h : 16 * g + 8 * h + 8, :] for g in range(4 * n // 16)], axis=0
        )
        for k in range(4):
            v = mix(v, entries[3 + k], 3 + k)
        total = total + jnp.sum((v * v).reshape(-1, 8, 128), axis=0)
        for g in range(4 * n // 16):
            back[16 * g + 8 * h : 16 * g + 8 * h + 8, :] = v[8 * g : 8 * (g + 1)]

    part_z[...] = jnp.sum(total, axis=0, keepdims=True)

    def small(source, target, slot, px, py, s_sem, r_sem):
        return pltpu.make_async_remote_copy(
            src_ref=source,
            dst_ref=target.at[slot],
            send_sem=s_sem,
            recv_sem=r_sem,
            device_id={"gx": px, "gy": py},
            device_id_type=MESH,
        )

    @pl.loop(1, n_z)
    def _(k):
        tz = (z + k) % n_z
        small(part_z, got_z, z, 2 * tz + core, gy, send_sems.at[2], got_z_sem.at[0]).start()

    got_z[z] = part_z[...]

    @pl.loop(0, n_z - 1)
    def _(t):
        tz = far_first(t)
        for i in range(plane):
            post(back, final, 1, tz, i)

    for i in range(plane):

        @pl.when(i != mine)
        def _():
            post(back, final, 1, z, i)

    keep(back, final)
    pltpu.make_async_copy(
        got_z.at[pl.ds(0, n_z - 1)], got_z.at[pl.ds(0, n_z - 1)], got_z_sem.at[0]
    ).wait()
    part_xc[...] = jnp.sum(got_z[...], axis=0)

    @pl.loop(1, 2 * n_x)
    def _(k):
        tc, tx = (core + k % 2) % 2, (gy + k // 2) % n_x
        small(part_xc, got_xc, mine, 2 * z + tc, tx, send_sems.at[3], got_xc_sem.at[0]).start()

    got_xc[mine] = part_xc[...]
    pltpu.make_async_copy(
        got_xc.at[pl.ds(0, 2 * n_x - 1)], got_xc.at[pl.ds(0, 2 * n_x - 1)], got_xc_sem.at[0]
    ).wait()
    summed = jnp.sum(jnp.sum(got_xc[...], axis=0), axis=1, keepdims=True)
    count = float(x_ref.shape[0] * x_ref.shape[1] * n)
    scale = lax.rsqrt(summed / count + EPSILON)
    arrived(back, final, 1)
    for n15 in range(2):
        for n7 in range(2):
            o_ref[pl.ds(n15 * 256 + n7, 128, stride=2), :] = (
                final[pl.ds(2 * n15 + n7, 128, stride=4), :] * scale
            )
    sent(send, held, 0)
    sent(back, final, 1)
    pltpu.make_async_copy(
        got_z.at[pl.ds(0, n_z - 1)], got_z.at[pl.ds(0, n_z - 1)], send_sems.at[2]
    ).wait()
    pltpu.make_async_copy(
        got_xc.at[pl.ds(0, 2 * n_x - 1)], got_xc.at[pl.ds(0, 2 * n_x - 1)], send_sems.at[3]
    ).wait()


def local(initial_state, fields, bond_order):
    amps = initial_state.shape[2]
    n = lax.axis_size("gx") * lax.axis_size("gy")
    n_z, n_xc = lax.axis_size("gx") // 2, 2 * lax.axis_size("gy")
    block = pltpu.VMEM((amps // 128, 128), jnp.float32)
    vmem, hbm = pl.BlockSpec(memory_space=pltpu.VMEM), pl.BlockSpec(memory_space=pltpu.HBM)
    pin = functools.partial(pltpu.with_memory_space_constraint, memory_space=pltpu.HBM)
    out = pl.pallas_call(
        kernel,
        out_shape=jax.ShapeDtypeStruct((amps // 128, 128), jnp.float32),
        in_specs=[hbm, hbm, hbm],
        out_specs=vmem,
        scratch_shapes=[
            pltpu.SMEM(fields.shape, jnp.float32),
            pltpu.SMEM(bond_order.shape, jnp.int32),
            block,
            block,
            block,
            block,
            block,
            block,
            pltpu.VMEM((1, 128), jnp.float32),
            pltpu.VMEM((1, 128), jnp.float32),
            pltpu.VMEM((n_z, 1, 128), jnp.float32),
            pltpu.VMEM((n_xc, 1, 128), jnp.float32),
            pltpu.SemaphoreType.DMA((4,)),
            pltpu.SemaphoreType.DMA((2,)),
            pltpu.SemaphoreType.DMA((1,)),
            pltpu.SemaphoreType.DMA((1,)),
            pltpu.SemaphoreType.DMA((3,)),
            pltpu.SemaphoreType.REGULAR((n_z + 2,)),
        ],
        compiler_params=pltpu.CompilerParams(
            collective_id=0, has_side_effects=True, vmem_limit_bytes=4 * 2**20
        ),
    )(
        pin(initial_state.reshape(amps // 128, 128)), pin(fields), pin(bond_order)
    )
    return out.reshape(initial_state.shape)


def solution(mesh):
    placed = (P(("groups", "gx"), "gy", None), P("groups"), P())
    return jax.shard_map(
        local,
        mesh=mesh,
        in_specs=placed,
        out_specs=P(("groups", "gx"), "gy", None),
        check_vma=False,
    )
```

```python
import functools

import jax
import jax.numpy as jnp
from jax import lax
from jax.experimental import pallas as pl
from jax.experimental.pallas import tpu as pltpu
from jax.sharding import PartitionSpec as P

MESH = pl.DeviceIdType.MESH
STEP = 0.15
BOOST = 1.161834242728283
EPSILON = 1e-06
STARTS = (0, 7, 9, 1)


def gate_entries(left, right, shape):
    left = jnp.full(shape, left, jnp.float32)
    right = jnp.full(shape, right, jnp.float32)
    half_sum = 0.5 * (left + right)
    half_diff = 0.5 * (left - right)
    radius = jnp.sqrt(half_diff * half_diff + 4.0)
    grow = jnp.exp(STEP * radius)
    decay = jnp.exp(-STEP * radius)
    cosine = 0.5 * (grow + decay)
    sine_ratio = 0.5 * (grow - decay) / radius
    low = jnp.exp(-STEP * (1.0 + half_sum))
    high = jnp.exp(-STEP * (1.0 - half_sum))
    up = BOOST * (cosine - sine_ratio * half_diff)
    down = BOOST * (cosine + sine_ratio * half_diff)
    flip = -2.0 * BOOST * sine_ratio
    return low, up, down, high, flip


def bond_step(matrix, fields, start, offset, lane):
    low, up, down, high, flip = gate_entries(
        fields[start + offset], fields[start + offset + 1], lane.shape
    )
    first = (lane >> offset) & 1
    second = (lane >> (offset + 1)) & 1
    zero = first == 0
    equal = first == second
    diagonal = jnp.where(equal, jnp.where(zero, low, high), jnp.where(zero, up, down))
    from_below = jnp.where(equal, 0.0, jnp.where(zero, flip, 0.0))
    from_above = jnp.where(equal, 0.0, jnp.where(zero, 0.0, flip))
    shift = jnp.left_shift(1, offset)
    return (
        matrix * diagonal
        + pltpu.roll(matrix, shift, 1) * from_below
        + pltpu.roll(matrix, 128 - shift, 1) * from_above
    )


def split(x):
    high = x.astype(jnp.bfloat16)
    return high, (x - high.astype(jnp.float32)).astype(jnp.bfloat16)


def dot(a, b):
    return jnp.dot(a, b, preferred_element_type=jnp.float32)


def dot_split(a, b):
    return dot(a[0], b[0]) + (dot(a[0], b[1]) + dot(a[1], b[0]))


def mix(value, entries, bit):
    low, up, down, high, flip = entries
    rows = value.shape[0]
    inner = 2**bit
    v = value.reshape(rows // (4 * inner), 2, 2, inner // 8, 8, 128)
    both0, only_first = v[:, 0, 0], v[:, 0, 1]
    only_second, both1 = v[:, 1, 0], v[:, 1, 1]
    new = jnp.stack(
        [
            jnp.stack([low * both0, down * only_first + flip * only_second], axis=1),
            jnp.stack([up * only_second + flip * only_first, high * both1], axis=1),
        ],
        axis=1,
    )
    return new.reshape(value.shape)


def kernel(
    x_hbm,
    fields_hbm,
    order_hbm,
    o_ref,
    fields,
    order,
    x_ref,
    t_ref,
    send,
    held,
    back,
    final,
    part_z,
    part_xc,
    got_z,
    got_xc,
    send_sems,
    recv_sems,
    got_z_sem,
    got_xc_sem,
    fetch_sems,
    ready,
):
    gx, gy = lax.axis_index("gx"), lax.axis_index("gy")
    n_z, n_x = lax.axis_size("gx") // 2, lax.axis_size("gy")
    plane = 2 * n_x
    n = n_z * plane
    z, core = gx // 2, gx % 2
    mine = core * n_x + gy
    me = z * plane + mine

    fetch = pltpu.make_async_copy(x_hbm, x_ref, fetch_sems.at[0])
    fetch_fields = pltpu.make_async_copy(fields_hbm, fields, fetch_sems.at[1])
    fetch_order = pltpu.make_async_copy(order_hbm, order, fetch_sems.at[2])
    fetch_fields.start()
    fetch_order.start()
    fetch.start()

    def at(tz, i):
        return {"gx": 2 * tz + i // n_x, "gy": i % n_x}

    def far_first(t):
        dz = n_z // 2 + ((t + 1) // 2) * (2 * (t % 2) - 1)
        return (z + dz + n_z) % n_z

    barrier = pltpu.get_barrier_semaphore()

    def greet(device):
        pl.semaphore_signal(barrier, inc=1, device_id=device, device_id_type=MESH)

    @pl.when(me > 0)
    def _():
        for i in range(plane):

            @pl.when((mine != i) & (z * plane + i > 0))
            def _():
                greet(at(z, i))

        greet(at(0, 0))

        @pl.loop(z + 1, n_z)
        def _(tz):
            for i in range(plane):
                greet(at(tz, i))

    lane = lax.broadcasted_iota(jnp.int32, (1, 128), 1)
    row = lax.broadcasted_iota(jnp.int32, (128, 128), 0)
    col = lax.broadcasted_iota(jnp.int32, (128, 128), 1)
    fetch_fields.wait()
    fetch_order.wait()
    identity = jnp.where(row == col, 1.0, 0.0)
    mats = [identity] * 4
    for e in range(6):
        for w in range(4):
            step = e if w in (0, 3) else 5 - e
            mats[w] = bond_step(mats[w], fields, STARTS[w], order[w, step], lane)
    w0t, w1, w2, w3t = [split(m) for m in mats]
    i0 = lax.broadcasted_iota(jnp.int32, (256, 128), 0)
    g0 = lax.broadcasted_iota(jnp.int32, (256, 128), 1)
    g1 = lax.broadcasted_iota(jnp.int32, (128, 256), 0)
    j1 = lax.broadcasted_iota(jnp.int32, (128, 256), 1)
    left = jnp.where((i0 >> 1) == g0, 1.0, 0.0).astype(jnp.bfloat16)
    right = jnp.where((j1 >> 1) == g1, 1.0, 0.0).astype(jnp.bfloat16)
    ii = lax.broadcasted_iota(jnp.int32, (256, 256), 0)
    jj = lax.broadcasted_iota(jnp.int32, (256, 256), 1)
    same = ((ii ^ jj) & 1) == 0
    w3k = [
        jnp.where(same, dot(dot(left, m).astype(jnp.bfloat16), right), 0.0).astype(jnp.bfloat16)
        for m in w3t
    ]

    @pl.when(me > 0)
    def _():
        pl.semaphore_wait(barrier, jnp.where(z > 0, (z + 1) * plane - 2, plane - 2))

        @pl.loop(0, n_z - 1)
        def _(t):
            tz = far_first(t)

            @pl.when((tz < z) & (tz * plane + mine > 0))
            def _():
                pl.semaphore_signal(
                    ready.at[z], inc=1, device_id=at(tz, mine), device_id_type=MESH
                )

    fetch.wait()
    for b in range(4):
        rows = slice(128 * b, 128 * (b + 1))
        y = dot_split(split(x_ref[rows, :]), w0t)
        t_ref[rows, :] = dot_split(w1, split(y))
    for n8 in range(2):
        ys = []
        for n7 in range(2):
            t = t_ref[pl.ds(n7 + 2 * n8, 128, stride=4), :]
            ys.append(dot_split(w2, split(t)))
        out = dot_split(split(jnp.concatenate(ys, axis=1)), w3k)
        for n15 in range(2):
            for n7 in range(2):
                send[pl.ds(4 * n8 + 2 * n15 + n7, 64, stride=8), :] = out[
                    64 * n15 : 64 * (n15 + 1), 128 * n7 : 128 * (n7 + 1)
                ]

    def post(source, target, which, tz, i):
        source, target = source.reshape(n, 4, 128), target.reshape(n, 4, 128)
        pltpu.make_async_remote_copy(
            src_ref=source.at[tz * plane + i],
            dst_ref=target.at[me],
            send_sem=send_sems.at[which],
            recv_sem=recv_sems.at[which],
            device_id=at(tz, i),
            device_id_type=MESH,
        ).start()

    def keep(source, target):
        source, target = source.reshape(n, 4, 128), target.reshape(n, 4, 128)
        target[me] = source[me]

    def post_known(tz):
        for i in range(plane):
            if i == 0:
                pl.when(tz > 0)(functools.partial(post, send, held, 0, tz, i))
            else:
                post(send, held, 0, tz, i)

    def arrived(source, target, which):
        part = pl.ds(0, 4 * (n - 1))
        copy = pltpu.make_async_copy(source.at[part], target.at[part], recv_sems.at[which])
        copy.wait()

    def sent(source, target, which):
        part = pl.ds(0, 4 * (n - 1))
        copy = pltpu.make_async_copy(source.at[part], target.at[part], send_sems.at[which])
        copy.wait()

    @pl.when(me == 0)
    def _():
        pl.semaphore_wait(barrier, n - 1)

    @pl.loop(0, n_z - 1)
    def _(t):
        tz = far_first(t)

        @pl.when((tz < z) & (me > 0))
        def _():
            post_known(tz)

        @pl.when(me == 0)
        def _():
            for i in range(plane):
                pl.semaphore_signal(
                    ready.at[n_z], inc=1, device_id=at(tz, i), device_id_type=MESH
                )
            for i in range(plane):
                post(send, held, 0, tz, i)

    @pl.when(me == 0)
    def _():
        for i in range(1, plane):
            pl.semaphore_signal(ready.at[n_z], inc=1, device_id=at(z, i), device_id_type=MESH)

    for i in range(plane):

        @pl.when((i != mine) & (z * plane + i > 0))
        def _():
            post(send, held, 0, z, i)

    @pl.when(me > 0)
    def _():
        @pl.loop(z + 1, n_z)
        def _(tz):
            pl.semaphore_wait(ready.at[tz], 1)
            post_known(tz)

        pl.semaphore_wait(ready.at[n_z], 1)
        post(send, held, 0, 0, 0)

    keep(send, held)
    entries = [
        gate_entries(fields[15 + k], fields[16 + k], (1, 128)) for k in range(7)
    ]
    srow = lax.broadcasted_iota(jnp.int32, (8, 128), 0)
    bit1, bit2 = (srow >> 1) & 1, (srow >> 2) & 1
    low, up, down, high, flip = entries[0]
    d15 = jnp.where(bit1 == bit2, jnp.where(bit1 == 0, low, high), jnp.where(bit1 == 0, up, down))
    f15 = jnp.where(bit1 == bit2, 0.0, flip)
    below15 = jnp.where(bit1 == 0, f15, 0.0)
    above15 = jnp.where(bit1 == 0, 0.0, f15)
    low, up, down, high, flip = entries[1]
    d16_0 = jnp.where(bit2 == 0, low, down)
    f16_0 = jnp.where(bit2 == 0, 0.0, flip)
    d16_1 = jnp.where(bit2 == 0, up, high)
    f16_1 = jnp.where(bit2 == 0, flip, 0.0)
    arrived(send, held, 0)

    for c in range(n // 8):
        v = held[32 * c : 32 * (c + 1), :].reshape(4, 8, 128)
        v = v * d15 + pltpu.roll(v, 2, 1) * below15 + pltpu.roll(v, 6, 1) * above15
        v = v.reshape(2, 2, 8, 128)
        v0, v1 = v[:, 0], v[:, 1]
        u0 = v0 * d16_0 + pltpu.roll(v1, 4, 1) * f16_0
        u1 = v1 * d16_1 + pltpu.roll(v0, 4, 1) * f16_1
        v = jnp.stack([u0, u1], axis=1).reshape(32, 128)
        t_ref[32 * c : 32 * (c + 1), :] = mix(v, entries[2], 3)
    total = jnp.zeros((8, 128), jnp.float32)
    for h in range(2):
        v = jnp.concatenate(
            [t_ref[16 * g + 8 * h : 16 * g + 8 * h + 8, :] for g in range(4 * n // 16)], axis=0
        )
        for k in range(4):
            v = mix(v, entries[3 + k], 3 + k)
        total = total + jnp.sum((v * v).reshape(-1, 8, 128), axis=0)
        for g in range(4 * n // 16):
            back[16 * g + 8 * h : 16 * g + 8 * h + 8, :] = v[8 * g : 8 * (g + 1)]

    part_z[...] = jnp.sum(total, axis=0, keepdims=True)

    def small(source, target, slot, px, py, s_sem, r_sem):
        return pltpu.make_async_remote_copy(
            src_ref=source,
            dst_ref=target.at[slot],
            send_sem=s_sem,
            recv_sem=r_sem,
            device_id={"gx": px, "gy": py},
            device_id_type=MESH,
        )

    @pl.loop(1, n_z)
    def _(k):
        tz = (z + k) % n_z
        small(part_z, got_z, z, 2 * tz + core, gy, send_sems.at[2], got_z_sem.at[0]).start()

    got_z[z] = part_z[...]

    @pl.loop(0, n_z - 1)
    def _(t):
        tz = far_first(t)
        for i in range(plane):
            post(back, final, 1, tz, i)

    for i in range(plane):

        @pl.when(i != mine)
        def _():
            post(back, final, 1, z, i)

    keep(back, final)
    pltpu.make_async_copy(
        got_z.at[pl.ds(0, n_z - 1)], got_z.at[pl.ds(0, n_z - 1)], got_z_sem.at[0]
    ).wait()
    part_xc[...] = jnp.sum(got_z[...], axis=0)

    @pl.loop(1, 2 * n_x)
    def _(k):
        tc, tx = (core + k % 2) % 2, (gy + k // 2) % n_x
        small(part_xc, got_xc, mine, 2 * z + tc, tx, send_sems.at[3], got_xc_sem.at[0]).start()

    got_xc[mine] = part_xc[...]
    pltpu.make_async_copy(
        got_xc.at[pl.ds(0, 2 * n_x - 1)], got_xc.at[pl.ds(0, 2 * n_x - 1)], got_xc_sem.at[0]
    ).wait()
    summed = jnp.sum(jnp.sum(got_xc[...], axis=0), axis=1, keepdims=True)
    count = float(x_ref.shape[0] * x_ref.shape[1] * n)
    scale = lax.rsqrt(summed / count + EPSILON)
    arrived(back, final, 1)
    for n15 in range(2):
        for n7 in range(2):
            o_ref[pl.ds(n15 * 256 + n7, 128, stride=2), :] = (
                final[pl.ds(2 * n15 + n7, 128, stride=4), :] * scale
            )
    sent(send, held, 0)
    sent(back, final, 1)
    pltpu.make_async_copy(
        got_z.at[pl.ds(0, n_z - 1)], got_z.at[pl.ds(0, n_z - 1)], send_sems.at[2]
    ).wait()
    pltpu.make_async_copy(
        got_xc.at[pl.ds(0, 2 * n_x - 1)], got_xc.at[pl.ds(0, 2 * n_x - 1)], send_sems.at[3]
    ).wait()


def local(initial_state, fields, bond_order):
    amps = initial_state.shape[2]
    n = lax.axis_size("gx") * lax.axis_size("gy")
    n_z, n_xc = lax.axis_size("gx") // 2, 2 * lax.axis_size("gy")
    block = pltpu.VMEM((amps // 128, 128), jnp.float32)
    vmem, hbm = pl.BlockSpec(memory_space=pltpu.VMEM), pl.BlockSpec(memory_space=pltpu.HBM)
    pin = functools.partial(pltpu.with_memory_space_constraint, memory_space=pltpu.HBM)
    out = pl.pallas_call(
        kernel,
        out_shape=jax.ShapeDtypeStruct((amps // 128, 128), jnp.float32),
        in_specs=[hbm, hbm, hbm],
        out_specs=vmem,
        scratch_shapes=[
            pltpu.SMEM(fields.shape, jnp.float32),
            pltpu.SMEM(bond_order.shape, jnp.int32),
            block,
            block,
            block,
            block,
            block,
            block,
            pltpu.VMEM((1, 128), jnp.float32),
            pltpu.VMEM((1, 128), jnp.float32),
            pltpu.VMEM((n_z, 1, 128), jnp.float32),
            pltpu.VMEM((n_xc, 1, 128), jnp.float32),
            pltpu.SemaphoreType.DMA((4,)),
            pltpu.SemaphoreType.DMA((2,)),
            pltpu.SemaphoreType.DMA((1,)),
            pltpu.SemaphoreType.DMA((1,)),
            pltpu.SemaphoreType.DMA((3,)),
            pltpu.SemaphoreType.REGULAR((n_z + 1,)),
        ],
        compiler_params=pltpu.CompilerParams(
            collective_id=0, has_side_effects=True, vmem_limit_bytes=4 * 2**20
        ),
    )(
        pin(initial_state.reshape(amps // 128, 128)), pin(fields), pin(bond_order)
    )
    return out.reshape(initial_state.shape)


def solution(mesh):
    placed = (P(("groups", "gx"), "gy", None), P("groups"), P())
    return jax.shard_map(
        local,
        mesh=mesh,
        in_specs=placed,
        out_specs=P(("groups", "gx"), "gy", None),
        check_vma=False,
    )
```

```python
import functools

import jax
import jax.numpy as jnp
from jax import lax
from jax.experimental import pallas as pl
from jax.experimental.pallas import tpu as pltpu
from jax.sharding import PartitionSpec as P

MESH = pl.DeviceIdType.MESH
STEP = 0.15
BOOST = 1.161834242728283
EPSILON = 1e-06
STARTS = (0, 7, 9, 1)
IDLE = 1


def gate_entries(left, right, shape):
    left = jnp.full(shape, left, jnp.float32)
    right = jnp.full(shape, right, jnp.float32)
    half_sum = 0.5 * (left + right)
    half_diff = 0.5 * (left - right)
    radius = jnp.sqrt(half_diff * half_diff + 4.0)
    grow = jnp.exp(STEP * radius)
    decay = jnp.exp(-STEP * radius)
    cosine = 0.5 * (grow + decay)
    sine_ratio = 0.5 * (grow - decay) / radius
    low = jnp.exp(-STEP * (1.0 + half_sum))
    high = jnp.exp(-STEP * (1.0 - half_sum))
    up = BOOST * (cosine - sine_ratio * half_diff)
    down = BOOST * (cosine + sine_ratio * half_diff)
    flip = -2.0 * BOOST * sine_ratio
    return low, up, down, high, flip


def bond_step(matrix, fields, start, offset, lane):
    low, up, down, high, flip = gate_entries(
        fields[start + offset], fields[start + offset + 1], lane.shape
    )
    first = (lane >> offset) & 1
    second = (lane >> (offset + 1)) & 1
    zero = first == 0
    equal = first == second
    diagonal = jnp.where(equal, jnp.where(zero, low, high), jnp.where(zero, up, down))
    from_below = jnp.where(equal, 0.0, jnp.where(zero, flip, 0.0))
    from_above = jnp.where(equal, 0.0, jnp.where(zero, 0.0, flip))
    shift = jnp.left_shift(1, offset)
    return (
        matrix * diagonal
        + pltpu.roll(matrix, shift, 1) * from_below
        + pltpu.roll(matrix, 128 - shift, 1) * from_above
    )


def split(x):
    high = x.astype(jnp.bfloat16)
    return high, (x - high.astype(jnp.float32)).astype(jnp.bfloat16)


def dot(a, b):
    return jnp.dot(a, b, preferred_element_type=jnp.float32)


def dot_split(a, b):
    return dot(a[0], b[0]) + (dot(a[0], b[1]) + dot(a[1], b[0]))


def mix(value, entries, bit):
    low, up, down, high, flip = entries
    rows = value.shape[0]
    inner = 2**bit
    v = value.reshape(rows // (4 * inner), 2, 2, inner // 8, 8, 128)
    both0, only_first = v[:, 0, 0], v[:, 0, 1]
    only_second, both1 = v[:, 1, 0], v[:, 1, 1]
    new = jnp.stack(
        [
            jnp.stack([low * both0, down * only_first + flip * only_second], axis=1),
            jnp.stack([up * only_second + flip * only_first, high * both1], axis=1),
        ],
        axis=1,
    )
    return new.reshape(value.shape)


def kernel(
    x_hbm,
    fields_hbm,
    order_hbm,
    o_ref,
    fields,
    order,
    x_ref,
    t_ref,
    send,
    held,
    back,
    final,
    part_z,
    part_xc,
    got_z,
    got_xc,
    send_sems,
    recv_sems,
    got_z_sem,
    got_xc_sem,
    fetch_sems,
    ready,
):
    gx, gy = lax.axis_index("gx"), lax.axis_index("gy")
    n_z, n_x = lax.axis_size("gx") // 2, lax.axis_size("gy")
    plane = 2 * n_x
    n = n_z * plane
    z, core = gx // 2, gx % 2
    mine = core * n_x + gy
    me = z * plane + mine

    fetch = pltpu.make_async_copy(x_hbm, x_ref, fetch_sems.at[0])
    fetch_fields = pltpu.make_async_copy(fields_hbm, fields, fetch_sems.at[1])
    fetch_order = pltpu.make_async_copy(order_hbm, order, fetch_sems.at[2])
    fetch_fields.start()
    fetch_order.start()
    fetch.start()

    def at(tz, i):
        return {"gx": 2 * tz + i // n_x, "gy": i % n_x}

    def far_first(t):
        dz = n_z // 2 + ((t + 1) // 2) * (2 * (t % 2) - 1)
        return (z + dz + n_z) % n_z

    busy = n_z - IDLE
    hosting = (z < busy) & (me > 0)
    extra_row = (z < IDLE) & (me > 0)
    extra_zero = (mine == 0) & (z == IDLE)
    extra_last = (mine == 0) & (z == IDLE + 1)
    double = extra_row | extra_zero | extra_last
    hosted = jnp.where(hosting, jnp.where(double, 2, 1), 0)
    second = jnp.where(
        extra_row, me + busy * plane, jnp.where(extra_last, busy * plane, 0)
    )
    barrier = pltpu.get_barrier_semaphore()

    def greet(device):
        pl.semaphore_signal(barrier, inc=1, device_id=device, device_id_type=MESH)

    @pl.when(hosting)
    def _():
        for i in range(plane):

            @pl.when((mine != i) & (z * plane + i > 0))
            def _():
                greet(at(z, i))

        greet(at(0, 0))

        @pl.loop(z + 1, n_z)
        def _(tz):
            for i in range(plane):
                greet(at(tz, i))

    got_z[...] = jnp.zeros_like(got_z)
    part_z[...] = jnp.zeros_like(part_z)
    lane = lax.broadcasted_iota(jnp.int32, (1, 128), 1)
    row = lax.broadcasted_iota(jnp.int32, (128, 128), 0)
    col = lax.broadcasted_iota(jnp.int32, (128, 128), 1)
    fetch_fields.wait()
    fetch_order.wait()
    identity = jnp.where(row == col, 1.0, 0.0)
    mats = [identity] * 4
    for e in range(6):
        for w in range(4):
            step = e if w in (0, 3) else 5 - e
            mats[w] = bond_step(mats[w], fields, STARTS[w], order[w, step], lane)
    w0t, w1, w2, w3t = [split(m) for m in mats]
    i0 = lax.broadcasted_iota(jnp.int32, (256, 128), 0)
    g0 = lax.broadcasted_iota(jnp.int32, (256, 128), 1)
    g1 = lax.broadcasted_iota(jnp.int32, (128, 256), 0)
    j1 = lax.broadcasted_iota(jnp.int32, (128, 256), 1)
    left = jnp.where((i0 >> 1) == g0, 1.0, 0.0).astype(jnp.bfloat16)
    right = jnp.where((j1 >> 1) == g1, 1.0, 0.0).astype(jnp.bfloat16)
    ii = lax.broadcasted_iota(jnp.int32, (256, 256), 0)
    jj = lax.broadcasted_iota(jnp.int32, (256, 256), 1)
    same = ((ii ^ jj) & 1) == 0
    w3k = [
        jnp.where(same, dot(dot(left, m).astype(jnp.bfloat16), right), 0.0).astype(jnp.bfloat16)
        for m in w3t
    ]

    @pl.when(hosting)
    def _():
        pl.semaphore_wait(barrier, jnp.where(z > 0, (z + 1) * plane - 2, plane - 2))

        @pl.loop(0, n_z - 1)
        def _(t):
            tz = far_first(t)

            @pl.when((tz < z) & (tz * plane + mine > 0))
            def _():
                pl.semaphore_signal(
                    ready.at[z], inc=1, device_id=at(tz, mine), device_id_type=MESH
                )

    @pl.when(jnp.logical_not(hosting))
    def _():
        pl.semaphore_wait(barrier, busy * plane - 1)

    fetch.wait()
    for b in range(4):
        rows = slice(128 * b, 128 * (b + 1))
        y = dot_split(split(x_ref[rows, :]), w0t)
        t_ref[rows, :] = dot_split(w1, split(y))
    for n8 in range(2):
        ys = []
        for n7 in range(2):
            t = t_ref[pl.ds(n7 + 2 * n8, 128, stride=4), :]
            ys.append(dot_split(w2, split(t)))
        out = dot_split(split(jnp.concatenate(ys, axis=1)), w3k)
        for n15 in range(2):
            for n7 in range(2):
                send[pl.ds(4 * n8 + 2 * n15 + n7, 64, stride=8), :] = out[
                    64 * n15 : 64 * (n15 + 1), 128 * n7 : 128 * (n7 + 1)
                ]

    def post(source, from_row, target, to_row, which, arrival, device):
        pltpu.make_async_remote_copy(
            src_ref=source.at[from_row],
            dst_ref=target.at[to_row],
            send_sem=send_sems.at[which],
            recv_sem=recv_sems.at[arrival],
            device_id=device,
            device_id_type=MESH,
        ).start()

    blocks = send.reshape(n, 4, 128)
    held_blocks = held.reshape(2 * n, 4, 128)
    back_blocks = back.reshape(2 * n, 4, 128)
    final_blocks = final.reshape(n, 4, 128)

    def give(row, slot, tz, i):
        post(blocks, row, held_blocks, slot * n + me, 0, slot, at(tz, i))

    def give_plane(tz):
        @pl.when(tz > 0)
        def _():
            give(tz * plane, 0, tz, 0)

        for i in range(1, plane):
            give(tz * plane + i, 0, tz, i)

        @pl.when(tz < IDLE)
        def _():
            if IDLE > 1:

                @pl.when(tz > 0)
                def _():
                    give((tz + busy) * plane, 1, tz, 0)

            for i in range(1, plane):
                give((tz + busy) * plane + i, 1, tz, i)

        @pl.when(tz == IDLE)
        def _():
            give(0, 1, tz, 0)

        @pl.when(tz == IDLE + 1)
        def _():
            give(busy * plane, 1, tz, 0)

    def await_blocks(semaphore, count):
        blocks_of = held_blocks.at[pl.ds(0, count)]
        pltpu.make_async_copy(blocks_of, blocks_of, semaphore).wait()

    @pl.loop(0, n_z - 1)
    def _(t):
        tz = far_first(t)

        @pl.when((tz < busy) & ((tz < z) | (me == 0)))
        def _():
            give_plane(tz)

    @pl.when(z < busy)
    def _():
        for i in range(plane):

            @pl.when((i != mine) & (z * plane + i > 0))
            def _():
                give(z * plane + i, 0, z, i)

                @pl.when(z < IDLE)
                def _():
                    give((z + busy) * plane + i, 1, z, i)

        @pl.when((mine > 0) & (z == IDLE))
        def _():
            give(0, 1, z, 0)

        @pl.when((mine > 0) & (z == IDLE + 1))
        def _():
            give(busy * plane, 1, z, 0)

    @pl.when(me > 0)
    def _():
        @pl.loop(z + 1, busy)
        def _(tz):
            pl.semaphore_wait(ready.at[tz], 1)
            give_plane(tz)

    @pl.when(hosting)
    def _():
        held_blocks[me] = blocks[me]

    @pl.when(double)
    def _():
        held_blocks[n + me] = blocks[second]

    entries = [
        gate_entries(fields[15 + k], fields[16 + k], (1, 128)) for k in range(7)
    ]
    srow = lax.broadcasted_iota(jnp.int32, (8, 128), 0)
    bit1, bit2 = (srow >> 1) & 1, (srow >> 2) & 1
    low, up, down, high, flip = entries[0]
    d15 = jnp.where(bit1 == bit2, jnp.where(bit1 == 0, low, high), jnp.where(bit1 == 0, up, down))
    f15 = jnp.where(bit1 == bit2, 0.0, flip)
    below15 = jnp.where(bit1 == 0, f15, 0.0)
    above15 = jnp.where(bit1 == 0, 0.0, f15)
    low, up, down, high, flip = entries[1]
    d16_0 = jnp.where(bit2 == 0, low, down)
    f16_0 = jnp.where(bit2 == 0, 0.0, flip)
    d16_1 = jnp.where(bit2 == 0, up, high)
    f16_1 = jnp.where(bit2 == 0, flip, 0.0)
    @pl.loop(0, hosted)
    def _(slot):
        await_blocks(recv_sems.at[slot], n - 1)
        for c in range(n // 8):
            v = held[pl.ds(pl.multiple_of(4 * n * slot + 32 * c, 32), 32), :].reshape(4, 8, 128)
            v = v * d15 + pltpu.roll(v, 2, 1) * below15 + pltpu.roll(v, 6, 1) * above15
            v = v.reshape(2, 2, 8, 128)
            v0, v1 = v[:, 0], v[:, 1]
            u0 = v0 * d16_0 + pltpu.roll(v1, 4, 1) * f16_0
            u1 = v1 * d16_1 + pltpu.roll(v0, 4, 1) * f16_1
            v = jnp.stack([u0, u1], axis=1).reshape(32, 128)
            t_ref[32 * c : 32 * (c + 1), :] = mix(v, entries[2], 3)
        total = jnp.zeros((8, 128), jnp.float32)
        for h in range(2):
            v = jnp.concatenate(
                [t_ref[16 * g + 8 * h : 16 * g + 8 * h + 8, :] for g in range(4 * n // 16)],
                axis=0,
            )
            for k in range(4):
                v = mix(v, entries[3 + k], 3 + k)
            total = total + jnp.sum((v * v).reshape(-1, 8, 128), axis=0)
            for g in range(4 * n // 16):
                rows = pl.ds(pl.multiple_of(4 * n * slot + 16 * g + 8 * h, 8), 8)
                back[rows, :] = v[8 * g : 8 * (g + 1)]
        part_z[...] += jnp.sum(total, axis=0, keepdims=True)

    def small(source, target, slot, px, py, s_sem, r_sem):
        return pltpu.make_async_remote_copy(
            src_ref=source,
            dst_ref=target.at[slot],
            send_sem=s_sem,
            recv_sem=r_sem,
            device_id={"gx": px, "gy": py},
            device_id_type=MESH,
        )

    @pl.when(hosting)
    def _():
        @pl.loop(1, n_z)
        def _(k):
            tz = (z + k) % n_z
            small(part_z, got_z, z, 2 * tz + core, gy, send_sems.at[2], got_z_sem.at[0]).start()

        got_z[z] = part_z[...]

    def give_back(slot, row, tz, i):
        post(back_blocks, slot * n + tz * plane + i, final_blocks, row, 1, 2, at(tz, i))

    @pl.when(hosting)
    def _():
        @pl.loop(0, n_z - 1)
        def _(t):
            tz = far_first(t)
            for i in range(plane):
                give_back(0, me, tz, i)

            @pl.when(double)
            def _():
                for i in range(plane):
                    give_back(1, second, tz, i)

        for i in range(plane):

            @pl.when(i != mine)
            def _():
                give_back(0, me, z, i)

                @pl.when(double)
                def _():
                    give_back(1, second, z, i)

        final_blocks[me] = back_blocks[me]

    @pl.when(double)
    def _():
        final_blocks[second] = back_blocks[n + me]

    def await_small(target, semaphore, count):
        rows = target.at[pl.ds(0, count)]
        pltpu.make_async_copy(rows, rows, semaphore).wait()

    others = busy - jnp.where(hosting, 1, 0) - jnp.where(mine == 0, 1, 0)
    for count in range(busy - 2, busy + 1):
        pl.when(others == count)(
            functools.partial(await_small, got_z, got_z_sem.at[0], count)
        )
    part_xc[...] = jnp.sum(got_z[...], axis=0)

    @pl.loop(1, 2 * n_x)
    def _(k):
        tc, tx = (core + k % 2) % 2, (gy + k // 2) % n_x
        small(part_xc, got_xc, mine, 2 * z + tc, tx, send_sems.at[3], got_xc_sem.at[0]).start()

    got_xc[mine] = part_xc[...]
    await_small(got_xc, got_xc_sem.at[0], plane - 1)
    summed = jnp.sum(jnp.sum(got_xc[...], axis=0), axis=1, keepdims=True)
    count = float(x_ref.shape[0] * x_ref.shape[1] * n)
    scale = lax.rsqrt(summed / count + EPSILON)
    for count in range(3):
        pl.when(hosted == count)(
            functools.partial(await_blocks, recv_sems.at[2], n - count)
        )
    for n15 in range(2):
        for n7 in range(2):
            o_ref[pl.ds(n15 * 256 + n7, 128, stride=2), :] = (
                final[pl.ds(2 * n15 + n7, 128, stride=4), :] * scale
            )
    for count in range(3):

        @pl.when(hosted == count)
        def _():
            await_blocks(send_sems.at[0], n - count)
            if count > 0:
                await_blocks(send_sems.at[1], count * (n - 1))
                await_small(got_z, send_sems.at[2], n_z - 1)

    await_small(got_xc, send_sems.at[3], plane - 1)


def local(initial_state, fields, bond_order):
    amps = initial_state.shape[2]
    n = lax.axis_size("gx") * lax.axis_size("gy")
    n_z, n_xc = lax.axis_size("gx") // 2, 2 * lax.axis_size("gy")
    block = pltpu.VMEM((amps // 128, 128), jnp.float32)
    slots = pltpu.VMEM((2 * amps // 128, 128), jnp.float32)
    vmem, hbm = pl.BlockSpec(memory_space=pltpu.VMEM), pl.BlockSpec(memory_space=pltpu.HBM)
    pin = functools.partial(pltpu.with_memory_space_constraint, memory_space=pltpu.HBM)
    out = pl.pallas_call(
        kernel,
        out_shape=jax.ShapeDtypeStruct((amps // 128, 128), jnp.float32),
        in_specs=[hbm, hbm, hbm],
        out_specs=vmem,
        scratch_shapes=[
            pltpu.SMEM(fields.shape, jnp.float32),
            pltpu.SMEM(bond_order.shape, jnp.int32),
            block,
            block,
            block,
            slots,
            slots,
            block,
            pltpu.VMEM((1, 128), jnp.float32),
            pltpu.VMEM((1, 128), jnp.float32),
            pltpu.VMEM((n_z, 1, 128), jnp.float32),
            pltpu.VMEM((n_xc, 1, 128), jnp.float32),
            pltpu.SemaphoreType.DMA((4,)),
            pltpu.SemaphoreType.DMA((3,)),
            pltpu.SemaphoreType.DMA((1,)),
            pltpu.SemaphoreType.DMA((1,)),
            pltpu.SemaphoreType.DMA((3,)),
            pltpu.SemaphoreType.REGULAR((n_z,)),
        ],
        compiler_params=pltpu.CompilerParams(
            collective_id=0, has_side_effects=True, vmem_limit_bytes=4 * 2**20
        ),
    )(
        pin(initial_state.reshape(amps // 128, 128)), pin(fields), pin(bond_order)
    )
    return out.reshape(initial_state.shape)


def solution(mesh):
    placed = (P(("groups", "gx"), "gy", None), P("groups"), P())
    return jax.shard_map(
        local,
        mesh=mesh,
        in_specs=placed,
        out_specs=P(("groups", "gx"), "gy", None),
        check_vma=False,
    )
```

```python
import functools

import jax
import jax.numpy as jnp
from jax import lax
from jax.experimental import pallas as pl
from jax.experimental.pallas import tpu as pltpu
from jax.sharding import PartitionSpec as P

MESH = pl.DeviceIdType.MESH
STEP = 0.15
BOOST = 1.161834242728283
EPSILON = 1e-06
STARTS = (0, 7, 9, 1)


def gate_entries(left, right, shape):
    left = jnp.full(shape, left, jnp.float32)
    right = jnp.full(shape, right, jnp.float32)
    half_sum = 0.5 * (left + right)
    half_diff = 0.5 * (left - right)
    radius = jnp.sqrt(half_diff * half_diff + 4.0)
    grow = jnp.exp(STEP * radius)
    decay = jnp.exp(-STEP * radius)
    cosine = 0.5 * (grow + decay)
    sine_ratio = 0.5 * (grow - decay) / radius
    low = jnp.exp(-STEP * (1.0 + half_sum))
    high = jnp.exp(-STEP * (1.0 - half_sum))
    up = BOOST * (cosine - sine_ratio * half_diff)
    down = BOOST * (cosine + sine_ratio * half_diff)
    flip = -2.0 * BOOST * sine_ratio
    return low, up, down, high, flip


def bond_step(matrix, fields, start, offset, lane):
    low, up, down, high, flip = gate_entries(
        fields[start + offset], fields[start + offset + 1], lane.shape
    )
    first = (lane >> offset) & 1
    second = (lane >> (offset + 1)) & 1
    zero = first == 0
    equal = first == second
    diagonal = jnp.where(equal, jnp.where(zero, low, high), jnp.where(zero, up, down))
    from_below = jnp.where(equal, 0.0, jnp.where(zero, flip, 0.0))
    from_above = jnp.where(equal, 0.0, jnp.where(zero, 0.0, flip))
    shift = jnp.left_shift(1, offset)
    return (
        matrix * diagonal
        + pltpu.roll(matrix, shift, 1) * from_below
        + pltpu.roll(matrix, 128 - shift, 1) * from_above
    )


def split(x):
    high = x.astype(jnp.bfloat16)
    return high, (x - high.astype(jnp.float32)).astype(jnp.bfloat16)


def dot(a, b):
    return jnp.dot(a, b, preferred_element_type=jnp.float32)


def dot_split(a, b):
    return dot(a[0], b[0]) + (dot(a[0], b[1]) + dot(a[1], b[0]))


def mix(value, entries, bit):
    low, up, down, high, flip = entries
    rows = value.shape[0]
    inner = 2**bit
    v = value.reshape(rows // (4 * inner), 2, 2, inner // 8, 8, 128)
    both0, only_first = v[:, 0, 0], v[:, 0, 1]
    only_second, both1 = v[:, 1, 0], v[:, 1, 1]
    new = jnp.stack(
        [
            jnp.stack([low * both0, down * only_first + flip * only_second], axis=1),
            jnp.stack([up * only_second + flip * only_first, high * both1], axis=1),
        ],
        axis=1,
    )
    return new.reshape(value.shape)


def kernel(
    x_hbm,
    fields_hbm,
    order_hbm,
    o_ref,
    fields,
    order,
    x_ref,
    t_ref,
    send,
    held,
    back,
    final,
    part_z,
    part_xc,
    got_z,
    got_xc,
    send_sems,
    recv_sems,
    got_z_sem,
    got_xc_sem,
    fetch_sems,
    ready,
):
    gx, gy = lax.axis_index("gx"), lax.axis_index("gy")
    n_z, n_x = lax.axis_size("gx") // 2, lax.axis_size("gy")
    plane = 2 * n_x
    n = n_z * plane
    z, core = gx // 2, gx % 2
    mine = core * n_x + gy
    me = z * plane + mine

    fetch = pltpu.make_async_copy(x_hbm, x_ref, fetch_sems.at[0])
    fetch_fields = pltpu.make_async_copy(fields_hbm, fields, fetch_sems.at[1])
    fetch_order = pltpu.make_async_copy(order_hbm, order, fetch_sems.at[2])
    fetch_fields.start()
    fetch_order.start()
    fetch.start()

    def at(tz, i):
        return {"gx": 2 * tz + i // n_x, "gy": i % n_x}

    def far_first(t):
        dz = n_z // 2 + ((t + 1) // 2) * (2 * (t % 2) - 1)
        return (z + dz + n_z) % n_z

    barrier = pltpu.get_barrier_semaphore()

    def greet(device):
        pl.semaphore_signal(barrier, inc=1, device_id=device, device_id_type=MESH)

    @pl.when(me > 0)
    def _():
        for i in range(plane):

            @pl.when((mine != i) & (z * plane + i > 0))
            def _():
                greet(at(z, i))

        greet(at(0, 0))

        @pl.loop(z + 1, n_z)
        def _(tz):
            for i in range(plane):
                greet(at(tz, i))

    @pl.when(me > 0)
    def _():
        pl.semaphore_wait(barrier, jnp.where(z > 0, (z + 1) * plane - 2, plane - 2))

        @pl.loop(0, n_z - 1)
        def _(t):
            tz = far_first(t)

            @pl.when((tz < z) & (tz * plane + mine > 0))
            def _():
                pl.semaphore_signal(
                    ready.at[z], inc=1, device_id=at(tz, mine), device_id_type=MESH
                )

    lane = lax.broadcasted_iota(jnp.int32, (1, 128), 1)
    row = lax.broadcasted_iota(jnp.int32, (128, 128), 0)
    col = lax.broadcasted_iota(jnp.int32, (128, 128), 1)
    fetch_fields.wait()
    fetch_order.wait()
    identity = jnp.where(row == col, 1.0, 0.0)
    mats = [identity] * 4
    for e in range(6):
        for w in range(4):
            step = e if w in (0, 3) else 5 - e
            mats[w] = bond_step(mats[w], fields, STARTS[w], order[w, step], lane)
    w0t, w1, w2, w3t = [split(m) for m in mats]
    i0 = lax.broadcasted_iota(jnp.int32, (256, 128), 0)
    g0 = lax.broadcasted_iota(jnp.int32, (256, 128), 1)
    g1 = lax.broadcasted_iota(jnp.int32, (128, 256), 0)
    j1 = lax.broadcasted_iota(jnp.int32, (128, 256), 1)
    left = jnp.where((i0 >> 1) == g0, 1.0, 0.0).astype(jnp.bfloat16)
    right = jnp.where((j1 >> 1) == g1, 1.0, 0.0).astype(jnp.bfloat16)
    ii = lax.broadcasted_iota(jnp.int32, (256, 256), 0)
    jj = lax.broadcasted_iota(jnp.int32, (256, 256), 1)
    same = ((ii ^ jj) & 1) == 0
    w3k = [
        jnp.where(same, dot(dot(left, m).astype(jnp.bfloat16), right), 0.0).astype(jnp.bfloat16)
        for m in w3t
    ]

    fetch.wait()
    for b in range(4):
        rows = slice(128 * b, 128 * (b + 1))
        y = dot_split(split(x_ref[rows, :]), w0t)
        t_ref[rows, :] = dot_split(w1, split(y))
    for n8 in range(2):
        ys = []
        for n7 in range(2):
            t = t_ref[pl.ds(n7 + 2 * n8, 128, stride=4), :]
            ys.append(dot_split(w2, split(t)))
        out = dot_split(split(jnp.concatenate(ys, axis=1)), w3k)
        for n15 in range(2):
            for n7 in range(2):
                send[pl.ds(4 * n8 + 2 * n15 + n7, 64, stride=8), :] = out[
                    64 * n15 : 64 * (n15 + 1), 128 * n7 : 128 * (n7 + 1)
                ]

    def post(source, target, which, tz, i):
        source, target = source.reshape(n, 4, 128), target.reshape(n, 4, 128)
        pltpu.make_async_remote_copy(
            src_ref=source.at[tz * plane + i],
            dst_ref=target.at[me],
            send_sem=send_sems.at[which],
            recv_sem=recv_sems.at[which],
            device_id=at(tz, i),
            device_id_type=MESH,
        ).start()

    def keep(source, target):
        source, target = source.reshape(n, 4, 128), target.reshape(n, 4, 128)
        target[me] = source[me]

    def post_known(tz):
        for i in range(plane):
            if i == 0:
                pl.when(tz > 0)(functools.partial(post, send, held, 0, tz, i))
            else:
                post(send, held, 0, tz, i)

    def arrived(source, target, which):
        part = pl.ds(0, 4 * (n - 1))
        copy = pltpu.make_async_copy(source.at[part], target.at[part], recv_sems.at[which])
        copy.wait()

    def sent(source, target, which):
        part = pl.ds(0, 4 * (n - 1))
        copy = pltpu.make_async_copy(source.at[part], target.at[part], send_sems.at[which])
        copy.wait()

    @pl.when(me == 0)
    def _():
        pl.semaphore_wait(barrier, n - 1)

        def ready_plane(tz, first):
            for i in range(first, plane):
                pl.semaphore_signal(
                    ready.at[n_z], inc=1, device_id=at(tz, i), device_id_type=MESH
                )

        @pl.loop(0, n_z - 1)
        def _(t):
            ready_plane(far_first(t), 0)

        ready_plane(z, 1)

    @pl.loop(0, n_z - 1)
    def _(t):
        tz = far_first(t)

        @pl.when((tz < z) | (me == 0))
        def _():
            post_known(tz)

    for i in range(plane):

        @pl.when((i != mine) & (z * plane + i > 0))
        def _():
            post(send, held, 0, z, i)

    @pl.when(me > 0)
    def _():
        @pl.loop(z + 1, n_z)
        def _(tz):
            pl.semaphore_wait(ready.at[tz], 1)
            post_known(tz)

        pl.semaphore_wait(ready.at[n_z], 1)
        post(send, held, 0, 0, 0)

    keep(send, held)
    entries = [
        gate_entries(fields[15 + k], fields[16 + k], (1, 128)) for k in range(7)
    ]
    srow = lax.broadcasted_iota(jnp.int32, (8, 128), 0)
    bit1, bit2 = (srow >> 1) & 1, (srow >> 2) & 1
    low, up, down, high, flip = entries[0]
    d15 = jnp.where(bit1 == bit2, jnp.where(bit1 == 0, low, high), jnp.where(bit1 == 0, up, down))
    f15 = jnp.where(bit1 == bit2, 0.0, flip)
    below15 = jnp.where(bit1 == 0, f15, 0.0)
    above15 = jnp.where(bit1 == 0, 0.0, f15)
    low, up, down, high, flip = entries[1]
    d16_0 = jnp.where(bit2 == 0, low, down)
    f16_0 = jnp.where(bit2 == 0, 0.0, flip)
    d16_1 = jnp.where(bit2 == 0, up, high)
    f16_1 = jnp.where(bit2 == 0, flip, 0.0)
    arrived(send, held, 0)

    for c in range(n // 8):
        v = held[32 * c : 32 * (c + 1), :].reshape(4, 8, 128)
        v = v * d15 + pltpu.roll(v, 2, 1) * below15 + pltpu.roll(v, 6, 1) * above15
        v = v.reshape(2, 2, 8, 128)
        v0, v1 = v[:, 0], v[:, 1]
        u0 = v0 * d16_0 + pltpu.roll(v1, 4, 1) * f16_0
        u1 = v1 * d16_1 + pltpu.roll(v0, 4, 1) * f16_1
        v = jnp.stack([u0, u1], axis=1).reshape(32, 128)
        t_ref[32 * c : 32 * (c + 1), :] = mix(v, entries[2], 3)
    total = jnp.zeros((8, 128), jnp.float32)
    for h in range(2):
        v = jnp.concatenate(
            [t_ref[16 * g + 8 * h : 16 * g + 8 * h + 8, :] for g in range(4 * n // 16)], axis=0
        )
        for k in range(4):
            v = mix(v, entries[3 + k], 3 + k)
        total = total + jnp.sum((v * v).reshape(-1, 8, 128), axis=0)
        for g in range(4 * n // 16):
            back[16 * g + 8 * h : 16 * g + 8 * h + 8, :] = v[8 * g : 8 * (g + 1)]

    part_z[...] = jnp.sum(total, axis=0, keepdims=True)

    def small(source, target, slot, px, py, s_sem, r_sem):
        return pltpu.make_async_remote_copy(
            src_ref=source,
            dst_ref=target.at[slot],
            send_sem=s_sem,
            recv_sem=r_sem,
            device_id={"gx": px, "gy": py},
            device_id_type=MESH,
        )

    @pl.loop(1, n_z)
    def _(k):
        tz = (z + k) % n_z
        small(part_z, got_z, z, 2 * tz + core, gy, send_sems.at[2], got_z_sem.at[0]).start()

    got_z[z] = part_z[...]

    @pl.loop(0, n_z - 1)
    def _(t):
        tz = far_first(t)
        for i in range(plane):
            post(back, final, 1, tz, i)

    for i in range(plane):

        @pl.when(i != mine)
        def _():
            post(back, final, 1, z, i)

    keep(back, final)
    pltpu.make_async_copy(
        got_z.at[pl.ds(0, n_z - 1)], got_z.at[pl.ds(0, n_z - 1)], got_z_sem.at[0]
    ).wait()
    part_xc[...] = jnp.sum(got_z[...], axis=0)

    @pl.loop(1, 2 * n_x)
    def _(k):
        tc, tx = (core + k % 2) % 2, (gy + k // 2) % n_x
        small(part_xc, got_xc, mine, 2 * z + tc, tx, send_sems.at[3], got_xc_sem.at[0]).start()

    got_xc[mine] = part_xc[...]
    pltpu.make_async_copy(
        got_xc.at[pl.ds(0, 2 * n_x - 1)], got_xc.at[pl.ds(0, 2 * n_x - 1)], got_xc_sem.at[0]
    ).wait()
    summed = jnp.sum(jnp.sum(got_xc[...], axis=0), axis=1, keepdims=True)
    count = float(x_ref.shape[0] * x_ref.shape[1] * n)
    scale = lax.rsqrt(summed / count + EPSILON)
    arrived(back, final, 1)
    for n15 in range(2):
        for n7 in range(2):
            o_ref[pl.ds(n15 * 256 + n7, 128, stride=2), :] = (
                final[pl.ds(2 * n15 + n7, 128, stride=4), :] * scale
            )
    sent(send, held, 0)
    sent(back, final, 1)
    pltpu.make_async_copy(
        got_z.at[pl.ds(0, n_z - 1)], got_z.at[pl.ds(0, n_z - 1)], send_sems.at[2]
    ).wait()
    pltpu.make_async_copy(
        got_xc.at[pl.ds(0, 2 * n_x - 1)], got_xc.at[pl.ds(0, 2 * n_x - 1)], send_sems.at[3]
    ).wait()


def local(initial_state, fields, bond_order):
    amps = initial_state.shape[2]
    n = lax.axis_size("gx") * lax.axis_size("gy")
    n_z, n_xc = lax.axis_size("gx") // 2, 2 * lax.axis_size("gy")
    block = pltpu.VMEM((amps // 128, 128), jnp.float32)
    vmem, hbm = pl.BlockSpec(memory_space=pltpu.VMEM), pl.BlockSpec(memory_space=pltpu.HBM)
    pin = functools.partial(pltpu.with_memory_space_constraint, memory_space=pltpu.HBM)
    out = pl.pallas_call(
        kernel,
        out_shape=jax.ShapeDtypeStruct((amps // 128, 128), jnp.float32),
        in_specs=[hbm, hbm, hbm],
        out_specs=vmem,
        scratch_shapes=[
            pltpu.SMEM(fields.shape, jnp.float32),
            pltpu.SMEM(bond_order.shape, jnp.int32),
            block,
            block,
            block,
            block,
            block,
            block,
            pltpu.VMEM((1, 128), jnp.float32),
            pltpu.VMEM((1, 128), jnp.float32),
            pltpu.VMEM((n_z, 1, 128), jnp.float32),
            pltpu.VMEM((n_xc, 1, 128), jnp.float32),
            pltpu.SemaphoreType.DMA((4,)),
            pltpu.SemaphoreType.DMA((2,)),
            pltpu.SemaphoreType.DMA((1,)),
            pltpu.SemaphoreType.DMA((1,)),
            pltpu.SemaphoreType.DMA((3,)),
            pltpu.SemaphoreType.REGULAR((n_z + 1,)),
        ],
        compiler_params=pltpu.CompilerParams(
            collective_id=0, has_side_effects=True, vmem_limit_bytes=4 * 2**20
        ),
    )(
        pin(initial_state.reshape(amps // 128, 128)), pin(fields), pin(bond_order)
    )
    return out.reshape(initial_state.shape)


def solution(mesh):
    placed = (P(("groups", "gx"), "gy", None), P("groups"), P())
    return jax.shard_map(
        local,
        mesh=mesh,
        in_specs=placed,
        out_specs=P(("groups", "gx"), "gy", None),
        check_vma=False,
    )
```

```python
import functools

import jax
import jax.numpy as jnp
from jax import lax
from jax.experimental import pallas as pl
from jax.experimental.pallas import tpu as pltpu
from jax.sharding import PartitionSpec as P

MESH = pl.DeviceIdType.MESH
STEP = 0.15
BOOST = 1.161834242728283
EPSILON = 1e-06
STARTS = (0, 7, 9, 1)


def gate_entries(left, right, shape):
    left = jnp.full(shape, left, jnp.float32)
    right = jnp.full(shape, right, jnp.float32)
    half_sum = 0.5 * (left + right)
    half_diff = 0.5 * (left - right)
    radius = jnp.sqrt(half_diff * half_diff + 4.0)
    grow = jnp.exp(STEP * radius)
    decay = jnp.exp(-STEP * radius)
    cosine = 0.5 * (grow + decay)
    sine_ratio = 0.5 * (grow - decay) / radius
    low = jnp.exp(-STEP * (1.0 + half_sum))
    high = jnp.exp(-STEP * (1.0 - half_sum))
    up = BOOST * (cosine - sine_ratio * half_diff)
    down = BOOST * (cosine + sine_ratio * half_diff)
    flip = -2.0 * BOOST * sine_ratio
    return low, up, down, high, flip


def bond_step(matrix, fields, start, offset, lane):
    low, up, down, high, flip = gate_entries(
        fields[start + offset], fields[start + offset + 1], lane.shape
    )
    first = (lane >> offset) & 1
    second = (lane >> (offset + 1)) & 1
    zero = first == 0
    equal = first == second
    diagonal = jnp.where(equal, jnp.where(zero, low, high), jnp.where(zero, up, down))
    from_below = jnp.where(equal, 0.0, jnp.where(zero, flip, 0.0))
    from_above = jnp.where(equal, 0.0, jnp.where(zero, 0.0, flip))
    shift = jnp.left_shift(1, offset)
    return (
        matrix * diagonal
        + pltpu.roll(matrix, shift, 1) * from_below
        + pltpu.roll(matrix, 128 - shift, 1) * from_above
    )


def split(x):
    high = x.astype(jnp.bfloat16)
    return high, (x - high.astype(jnp.float32)).astype(jnp.bfloat16)


def dot(a, b):
    return jnp.dot(a, b, preferred_element_type=jnp.float32)


def dot_split(a, b):
    return dot(a[0], b[0]) + (dot(a[0], b[1]) + dot(a[1], b[0]))


def mix(value, entries, bit):
    low, up, down, high, flip = entries
    rows = value.shape[0]
    inner = 2**bit
    v = value.reshape(rows // (4 * inner), 2, 2, inner // 8, 8, 128)
    both0, only_first = v[:, 0, 0], v[:, 0, 1]
    only_second, both1 = v[:, 1, 0], v[:, 1, 1]
    new = jnp.stack(
        [
            jnp.stack([low * both0, down * only_first + flip * only_second], axis=1),
            jnp.stack([up * only_second + flip * only_first, high * both1], axis=1),
        ],
        axis=1,
    )
    return new.reshape(value.shape)


def kernel(
    x_hbm,
    fields_hbm,
    order_hbm,
    o_ref,
    fields,
    order,
    x_ref,
    t_ref,
    send,
    held,
    back,
    final,
    part_z,
    part_xc,
    got_z,
    got_xc,
    send_sems,
    recv_sems,
    got_z_sem,
    got_xc_sem,
    fetch_sems,
    ready,
):
    gx, gy = lax.axis_index("gx"), lax.axis_index("gy")
    n_z, n_x = lax.axis_size("gx") // 2, lax.axis_size("gy")
    plane = 2 * n_x
    n = n_z * plane
    z, core = gx // 2, gx % 2
    mine = core * n_x + gy
    me = z * plane + mine

    fetch = pltpu.make_async_copy(x_hbm, x_ref, fetch_sems.at[0])
    fetch_fields = pltpu.make_async_copy(fields_hbm, fields, fetch_sems.at[1])
    fetch_order = pltpu.make_async_copy(order_hbm, order, fetch_sems.at[2])
    fetch_fields.start()
    fetch_order.start()
    fetch.start()

    def at(tz, i):
        return {"gx": 2 * tz + i // n_x, "gy": i % n_x}

    def far_first(t):
        dz = n_z // 2 + ((t + 1) // 2) * (2 * (t % 2) - 1)
        return (z + dz + n_z) % n_z

    barrier = pltpu.get_barrier_semaphore()

    def greet(device):
        pl.semaphore_signal(barrier, inc=1, device_id=device, device_id_type=MESH)

    @pl.when(me > 0)
    def _():
        for i in range(plane):

            @pl.when((mine != i) & (z * plane + i > 0))
            def _():
                greet(at(z, i))

        greet(at(0, 0))

        @pl.loop(z + 1, n_z)
        def _(tz):
            for i in range(plane):
                greet(at(tz, i))

    lane = lax.broadcasted_iota(jnp.int32, (1, 128), 1)
    row = lax.broadcasted_iota(jnp.int32, (128, 128), 0)
    col = lax.broadcasted_iota(jnp.int32, (128, 128), 1)
    fetch_fields.wait()
    fetch_order.wait()
    identity = jnp.where(row == col, 1.0, 0.0)
    mats = [identity] * 4
    for e in range(6):
        for w in range(4):
            step = e if w in (0, 3) else 5 - e
            mats[w] = bond_step(mats[w], fields, STARTS[w], order[w, step], lane)
    w0t, w1, w2, w3t = [split(m) for m in mats]
    i0 = lax.broadcasted_iota(jnp.int32, (256, 128), 0)
    g0 = lax.broadcasted_iota(jnp.int32, (256, 128), 1)
    g1 = lax.broadcasted_iota(jnp.int32, (128, 256), 0)
    j1 = lax.broadcasted_iota(jnp.int32, (128, 256), 1)
    left = jnp.where((i0 >> 1) == g0, 1.0, 0.0).astype(jnp.bfloat16)
    right = jnp.where((j1 >> 1) == g1, 1.0, 0.0).astype(jnp.bfloat16)
    ii = lax.broadcasted_iota(jnp.int32, (256, 256), 0)
    jj = lax.broadcasted_iota(jnp.int32, (256, 256), 1)
    same = ((ii ^ jj) & 1) == 0
    w3k = [
        jnp.where(same, dot(dot(left, m).astype(jnp.bfloat16), right), 0.0).astype(jnp.bfloat16)
        for m in w3t
    ]

    fetch.wait()
    for b in range(4):
        rows = slice(128 * b, 128 * (b + 1))
        y = dot_split(split(x_ref[rows, :]), w0t)
        t_ref[rows, :] = dot_split(w1, split(y))
    for n8 in range(2):
        ys = []
        for n7 in range(2):
            t = t_ref[pl.ds(n7 + 2 * n8, 128, stride=4), :]
            ys.append(dot_split(w2, split(t)))
        out = dot_split(split(jnp.concatenate(ys, axis=1)), w3k)
        for n15 in range(2):
            for n7 in range(2):
                send[pl.ds(4 * n8 + 2 * n15 + n7, 64, stride=8), :] = out[
                    64 * n15 : 64 * (n15 + 1), 128 * n7 : 128 * (n7 + 1)
                ]

    @pl.when(me > 0)
    def _():
        pl.semaphore_wait(barrier, jnp.where(z > 0, (z + 1) * plane - 2, plane - 2))

        @pl.loop(0, n_z - 1)
        def _(t):
            tz = far_first(t)

            @pl.when((tz < z) & (tz * plane + mine > 0))
            def _():
                pl.semaphore_signal(
                    ready.at[z], inc=1, device_id=at(tz, mine), device_id_type=MESH
                )

    def post(source, target, which, tz, i):
        source, target = source.reshape(n, 4, 128), target.reshape(n, 4, 128)
        pltpu.make_async_remote_copy(
            src_ref=source.at[tz * plane + i],
            dst_ref=target.at[me],
            send_sem=send_sems.at[which],
            recv_sem=recv_sems.at[which],
            device_id=at(tz, i),
            device_id_type=MESH,
        ).start()

    def keep(source, target):
        source, target = source.reshape(n, 4, 128), target.reshape(n, 4, 128)
        target[me] = source[me]

    def post_known(tz):
        for i in range(plane):
            if i == 0:
                pl.when(tz > 0)(functools.partial(post, send, held, 0, tz, i))
            else:
                post(send, held, 0, tz, i)

    def arrived(source, target, which):
        part = pl.ds(0, 4 * (n - 1))
        copy = pltpu.make_async_copy(source.at[part], target.at[part], recv_sems.at[which])
        copy.wait()

    def sent(source, target, which):
        part = pl.ds(0, 4 * (n - 1))
        copy = pltpu.make_async_copy(source.at[part], target.at[part], send_sems.at[which])
        copy.wait()

    @pl.when(me == 0)
    def _():
        pl.semaphore_wait(barrier, n - 1)

    @pl.loop(0, n_z - 1)
    def _(t):
        tz = far_first(t)

        @pl.when((tz < z) & (me > 0))
        def _():
            post_known(tz)

        @pl.when(me == 0)
        def _():
            for i in range(plane):
                pl.semaphore_signal(
                    ready.at[n_z], inc=1, device_id=at(tz, i), device_id_type=MESH
                )
            for i in range(plane):
                post(send, held, 0, tz, i)

    @pl.when(me == 0)
    def _():
        for i in range(1, plane):
            pl.semaphore_signal(ready.at[n_z], inc=1, device_id=at(z, i), device_id_type=MESH)

    for i in range(plane):

        @pl.when((i != mine) & (z * plane + i > 0))
        def _():
            post(send, held, 0, z, i)

    @pl.when(me > 0)
    def _():
        @pl.loop(z + 1, n_z)
        def _(tz):
            pl.semaphore_wait(ready.at[tz], 1)
            post_known(tz)

        pl.semaphore_wait(ready.at[n_z], 1)
        post(send, held, 0, 0, 0)

    keep(send, held)
    entries = [
        gate_entries(fields[15 + k], fields[16 + k], (1, 128)) for k in range(7)
    ]
    srow = lax.broadcasted_iota(jnp.int32, (8, 128), 0)
    bit1, bit2 = (srow >> 1) & 1, (srow >> 2) & 1
    low, up, down, high, flip = entries[0]
    d15 = jnp.where(bit1 == bit2, jnp.where(bit1 == 0, low, high), jnp.where(bit1 == 0, up, down))
    f15 = jnp.where(bit1 == bit2, 0.0, flip)
    below15 = jnp.where(bit1 == 0, f15, 0.0)
    above15 = jnp.where(bit1 == 0, 0.0, f15)
    low, up, down, high, flip = entries[1]
    d16_0 = jnp.where(bit2 == 0, low, down)
    f16_0 = jnp.where(bit2 == 0, 0.0, flip)
    d16_1 = jnp.where(bit2 == 0, up, high)
    f16_1 = jnp.where(bit2 == 0, flip, 0.0)
    arrived(send, held, 0)

    for c in range(n // 8):
        v = held[32 * c : 32 * (c + 1), :].reshape(4, 8, 128)
        v = v * d15 + pltpu.roll(v, 2, 1) * below15 + pltpu.roll(v, 6, 1) * above15
        v = v.reshape(2, 2, 8, 128)
        v0, v1 = v[:, 0], v[:, 1]
        u0 = v0 * d16_0 + pltpu.roll(v1, 4, 1) * f16_0
        u1 = v1 * d16_1 + pltpu.roll(v0, 4, 1) * f16_1
        v = jnp.stack([u0, u1], axis=1).reshape(32, 128)
        t_ref[32 * c : 32 * (c + 1), :] = mix(v, entries[2], 3)
    total = jnp.zeros((8, 128), jnp.float32)
    for h in range(2):
        v = jnp.concatenate(
            [t_ref[16 * g + 8 * h : 16 * g + 8 * h + 8, :] for g in range(4 * n // 16)], axis=0
        )
        for k in range(4):
            v = mix(v, entries[3 + k], 3 + k)
        total = total + jnp.sum((v * v).reshape(-1, 8, 128), axis=0)
        for g in range(4 * n // 16):
            back[16 * g + 8 * h : 16 * g + 8 * h + 8, :] = v[8 * g : 8 * (g + 1)]

    part_z[...] = jnp.sum(total, axis=0, keepdims=True)

    def small(source, target, slot, px, py, s_sem, r_sem):
        return pltpu.make_async_remote_copy(
            src_ref=source,
            dst_ref=target.at[slot],
            send_sem=s_sem,
            recv_sem=r_sem,
            device_id={"gx": px, "gy": py},
            device_id_type=MESH,
        )

    @pl.loop(1, n_z)
    def _(k):
        tz = (z + k) % n_z
        small(part_z, got_z, z, 2 * tz + core, gy, send_sems.at[2], got_z_sem.at[0]).start()

    got_z[z] = part_z[...]

    @pl.loop(0, n_z - 1)
    def _(t):
        tz = far_first(t)
        for i in range(plane):
            post(back, final, 1, tz, i)

    for i in range(plane):

        @pl.when(i != mine)
        def _():
            post(back, final, 1, z, i)

    keep(back, final)
    pltpu.make_async_copy(
        got_z.at[pl.ds(0, n_z - 1)], got_z.at[pl.ds(0, n_z - 1)], got_z_sem.at[0]
    ).wait()
    part_xc[...] = jnp.sum(got_z[...], axis=0)

    @pl.loop(1, 2 * n_x)
    def _(k):
        tc, tx = (core + k % 2) % 2, (gy + k // 2) % n_x
        small(part_xc, got_xc, mine, 2 * z + tc, tx, send_sems.at[3], got_xc_sem.at[0]).start()

    got_xc[mine] = part_xc[...]
    pltpu.make_async_copy(
        got_xc.at[pl.ds(0, 2 * n_x - 1)], got_xc.at[pl.ds(0, 2 * n_x - 1)], got_xc_sem.at[0]
    ).wait()
    summed = jnp.sum(jnp.sum(got_xc[...], axis=0), axis=1, keepdims=True)
    count = float(x_ref.shape[0] * x_ref.shape[1] * n)
    scale = lax.rsqrt(summed / count + EPSILON)
    arrived(back, final, 1)
    for n15 in range(2):
        for n7 in range(2):
            o_ref[pl.ds(n15 * 256 + n7, 128, stride=2), :] = (
                final[pl.ds(2 * n15 + n7, 128, stride=4), :] * scale
            )
    sent(send, held, 0)
    sent(back, final, 1)
    pltpu.make_async_copy(
        got_z.at[pl.ds(0, n_z - 1)], got_z.at[pl.ds(0, n_z - 1)], send_sems.at[2]
    ).wait()
    pltpu.make_async_copy(
        got_xc.at[pl.ds(0, 2 * n_x - 1)], got_xc.at[pl.ds(0, 2 * n_x - 1)], send_sems.at[3]
    ).wait()


def local(initial_state, fields, bond_order):
    amps = initial_state.shape[2]
    n = lax.axis_size("gx") * lax.axis_size("gy")
    n_z, n_xc = lax.axis_size("gx") // 2, 2 * lax.axis_size("gy")
    block = pltpu.VMEM((amps // 128, 128), jnp.float32)
    vmem, hbm = pl.BlockSpec(memory_space=pltpu.VMEM), pl.BlockSpec(memory_space=pltpu.HBM)
    pin = functools.partial(pltpu.with_memory_space_constraint, memory_space=pltpu.HBM)
    out = pl.pallas_call(
        kernel,
        out_shape=jax.ShapeDtypeStruct((amps // 128, 128), jnp.float32),
        in_specs=[hbm, hbm, hbm],
        out_specs=vmem,
        scratch_shapes=[
            pltpu.SMEM(fields.shape, jnp.float32),
            pltpu.SMEM(bond_order.shape, jnp.int32),
            block,
            block,
            block,
            block,
            block,
            block,
            pltpu.VMEM((1, 128), jnp.float32),
            pltpu.VMEM((1, 128), jnp.float32),
            pltpu.VMEM((n_z, 1, 128), jnp.float32),
            pltpu.VMEM((n_xc, 1, 128), jnp.float32),
            pltpu.SemaphoreType.DMA((4,)),
            pltpu.SemaphoreType.DMA((2,)),
            pltpu.SemaphoreType.DMA((1,)),
            pltpu.SemaphoreType.DMA((1,)),
            pltpu.SemaphoreType.DMA((3,)),
            pltpu.SemaphoreType.REGULAR((n_z + 1,)),
        ],
        compiler_params=pltpu.CompilerParams(
            collective_id=0, has_side_effects=True, vmem_limit_bytes=4 * 2**20
        ),
    )(
        pin(initial_state.reshape(amps // 128, 128)), pin(fields), pin(bond_order)
    )
    return out.reshape(initial_state.shape)


def solution(mesh):
    placed = (P(("groups", "gx"), "gy", None), P("groups"), P())
    return jax.shard_map(
        local,
        mesh=mesh,
        in_specs=placed,
        out_specs=P(("groups", "gx"), "gy", None),
        check_vma=False,
    )
```

```python
import functools

import jax
import jax.numpy as jnp
from jax import lax
from jax.experimental import pallas as pl
from jax.experimental.pallas import tpu as pltpu
from jax.sharding import PartitionSpec as P

MESH = pl.DeviceIdType.MESH
STEP = 0.15
BOOST = 1.161834242728283
EPSILON = 1e-06
STARTS = (0, 7, 9, 1)


def gate_entries(left, right, shape):
    left = jnp.full(shape, left, jnp.float32)
    right = jnp.full(shape, right, jnp.float32)
    half_sum = 0.5 * (left + right)
    half_diff = 0.5 * (left - right)
    radius = jnp.sqrt(half_diff * half_diff + 4.0)
    grow = jnp.exp(STEP * radius)
    decay = jnp.exp(-STEP * radius)
    cosine = 0.5 * (grow + decay)
    sine_ratio = 0.5 * (grow - decay) / radius
    low = jnp.exp(-STEP * (1.0 + half_sum))
    high = jnp.exp(-STEP * (1.0 - half_sum))
    up = BOOST * (cosine - sine_ratio * half_diff)
    down = BOOST * (cosine + sine_ratio * half_diff)
    flip = -2.0 * BOOST * sine_ratio
    return low, up, down, high, flip


def bond_step(matrix, fields, start, offset, lane):
    low, up, down, high, flip = gate_entries(
        fields[start + offset], fields[start + offset + 1], lane.shape
    )
    first = (lane >> offset) & 1
    second = (lane >> (offset + 1)) & 1
    zero = first == 0
    equal = first == second
    diagonal = jnp.where(equal, jnp.where(zero, low, high), jnp.where(zero, up, down))
    from_below = jnp.where(equal, 0.0, jnp.where(zero, flip, 0.0))
    from_above = jnp.where(equal, 0.0, jnp.where(zero, 0.0, flip))
    shift = jnp.left_shift(1, offset)
    if matrix is None:
        row = lax.broadcasted_iota(jnp.int32, (128, 128), 0)
        col = lax.broadcasted_iota(jnp.int32, (128, 128), 1)
        moved = jnp.where(row == col - shift, from_below, 0.0)
        moved = jnp.where(row == col + shift, from_above, moved)
        return jnp.where(row == col, diagonal, moved)
    return (
        matrix * diagonal
        + pltpu.roll(matrix, shift, 1) * from_below
        + pltpu.roll(matrix, 128 - shift, 1) * from_above
    )


def split(x):
    high = x.astype(jnp.bfloat16)
    return high, (x - high.astype(jnp.float32)).astype(jnp.bfloat16)


def dot(a, b):
    return jnp.dot(a, b, preferred_element_type=jnp.float32)


def dot_split(a, b):
    return dot(a[0], b[0]) + (dot(a[0], b[1]) + dot(a[1], b[0]))


def mix(value, entries, bit):
    low, up, down, high, flip = entries
    rows = value.shape[0]
    inner = 2**bit
    v = value.reshape(rows // (4 * inner), 2, 2, inner // 8, 8, 128)
    both0, only_first = v[:, 0, 0], v[:, 0, 1]
    only_second, both1 = v[:, 1, 0], v[:, 1, 1]
    new = jnp.stack(
        [
            jnp.stack([low * both0, down * only_first + flip * only_second], axis=1),
            jnp.stack([up * only_second + flip * only_first, high * both1], axis=1),
        ],
        axis=1,
    )
    return new.reshape(value.shape)


def kernel(
    x_hbm,
    fields_hbm,
    order_hbm,
    o_ref,
    fields,
    order,
    x_ref,
    t_ref,
    send,
    held,
    back,
    final,
    part_z,
    part_xc,
    got_z,
    got_xc,
    send_sems,
    recv_sems,
    got_z_sem,
    got_xc_sem,
    fetch_sems,
    ready,
):
    gx, gy = lax.axis_index("gx"), lax.axis_index("gy")
    n_z, n_x = lax.axis_size("gx") // 2, lax.axis_size("gy")
    plane = 2 * n_x
    n = n_z * plane
    z, core = gx // 2, gx % 2
    mine = core * n_x + gy
    me = z * plane + mine

    fetch = pltpu.make_async_copy(x_hbm, x_ref, fetch_sems.at[0])
    fetch_fields = pltpu.make_async_copy(fields_hbm, fields, fetch_sems.at[1])
    fetch_order = pltpu.make_async_copy(order_hbm, order, fetch_sems.at[2])
    fetch_fields.start()
    fetch_order.start()
    fetch.start()

    def at(tz, i):
        return {"gx": 2 * tz + i // n_x, "gy": i % n_x}

    def far_first(t):
        dz = n_z // 2 + ((t + 1) // 2) * (2 * (t % 2) - 1)
        return (z + dz + n_z) % n_z

    barrier = pltpu.get_barrier_semaphore()

    def greet(device):
        pl.semaphore_signal(barrier, inc=1, device_id=device, device_id_type=MESH)

    @pl.when(me > 0)
    def _():
        for i in range(plane):

            @pl.when((mine != i) & (z * plane + i > 0))
            def _():
                greet(at(z, i))

        greet(at(0, 0))

        @pl.loop(z + 1, n_z)
        def _(tz):
            for i in range(plane):
                greet(at(tz, i))

    lane = lax.broadcasted_iota(jnp.int32, (1, 128), 1)
    fetch_fields.wait()
    fetch_order.wait()
    mats = [None] * 4
    for e in range(6):
        for w in range(4):
            step = e if w in (0, 3) else 5 - e
            mats[w] = bond_step(mats[w], fields, STARTS[w], order[w, step], lane)
    w0t, w1, w2, w3t = [split(m) for m in mats]
    i0 = lax.broadcasted_iota(jnp.int32, (256, 128), 0)
    g0 = lax.broadcasted_iota(jnp.int32, (256, 128), 1)
    g1 = lax.broadcasted_iota(jnp.int32, (128, 256), 0)
    j1 = lax.broadcasted_iota(jnp.int32, (128, 256), 1)
    left = jnp.where((i0 >> 1) == g0, 1.0, 0.0).astype(jnp.bfloat16)
    right = jnp.where((j1 >> 1) == g1, 1.0, 0.0).astype(jnp.bfloat16)
    ii = lax.broadcasted_iota(jnp.int32, (256, 256), 0)
    jj = lax.broadcasted_iota(jnp.int32, (256, 256), 1)
    same = ((ii ^ jj) & 1) == 0
    w3k = [
        jnp.where(same, dot(dot(left, m).astype(jnp.bfloat16), right), 0.0).astype(jnp.bfloat16)
        for m in w3t
    ]

    @pl.when(me > 0)
    def _():
        pl.semaphore_wait(barrier, jnp.where(z > 0, (z + 1) * plane - 2, plane - 2))

        @pl.loop(0, n_z - 1)
        def _(t):
            tz = far_first(t)

            @pl.when((tz < z) & (tz * plane + mine > 0))
            def _():
                pl.semaphore_signal(
                    ready.at[z], inc=1, device_id=at(tz, mine), device_id_type=MESH
                )

    fetch.wait()
    for b in range(4):
        rows = slice(128 * b, 128 * (b + 1))
        y = dot_split(split(x_ref[rows, :]), w0t)
        t_ref[rows, :] = dot_split(w1, split(y))
    for n8 in range(2):
        ys = []
        for n7 in range(2):
            t = t_ref[pl.ds(n7 + 2 * n8, 128, stride=4), :]
            ys.append(dot_split(w2, split(t)))
        out = dot_split(split(jnp.concatenate(ys, axis=1)), w3k)
        for n15 in range(2):
            for n7 in range(2):
                send[pl.ds(4 * n8 + 2 * n15 + n7, 64, stride=8), :] = out[
                    64 * n15 : 64 * (n15 + 1), 128 * n7 : 128 * (n7 + 1)
                ]

    def post(source, target, which, tz, i):
        source, target = source.reshape(n, 4, 128), target.reshape(n, 4, 128)
        pltpu.make_async_remote_copy(
            src_ref=source.at[tz * plane + i],
            dst_ref=target.at[me],
            send_sem=send_sems.at[which],
            recv_sem=recv_sems.at[which],
            device_id=at(tz, i),
            device_id_type=MESH,
        ).start()

    def keep(source, target):
        source, target = source.reshape(n, 4, 128), target.reshape(n, 4, 128)
        target[me] = source[me]

    def post_known(tz):
        for i in range(plane):
            if i == 0:
                pl.when(tz > 0)(functools.partial(post, send, held, 0, tz, i))
            else:
                post(send, held, 0, tz, i)

    def arrived(source, target, which):
        part = pl.ds(0, 4 * (n - 1))
        copy = pltpu.make_async_copy(source.at[part], target.at[part], recv_sems.at[which])
        copy.wait()

    def sent(source, target, which):
        part = pl.ds(0, 4 * (n - 1))
        copy = pltpu.make_async_copy(source.at[part], target.at[part], send_sems.at[which])
        copy.wait()

    @pl.when(me == 0)
    def _():
        pl.semaphore_wait(barrier, n - 1)

    @pl.loop(0, n_z - 1)
    def _(t):
        tz = far_first(t)

        @pl.when((tz < z) & (me > 0))
        def _():
            post_known(tz)

        @pl.when(me == 0)
        def _():
            for i in range(plane):
                pl.semaphore_signal(
                    ready.at[n_z], inc=1, device_id=at(tz, i), device_id_type=MESH
                )
            for i in range(plane):
                post(send, held, 0, tz, i)

    @pl.when(me == 0)
    def _():
        for i in range(1, plane):
            pl.semaphore_signal(ready.at[n_z], inc=1, device_id=at(z, i), device_id_type=MESH)

    for i in range(plane):

        @pl.when((i != mine) & (z * plane + i > 0))
        def _():
            post(send, held, 0, z, i)

    @pl.when(me > 0)
    def _():
        @pl.loop(z + 1, n_z)
        def _(tz):
            pl.semaphore_wait(ready.at[tz], 1)
            post_known(tz)

        pl.semaphore_wait(ready.at[n_z], 1)
        post(send, held, 0, 0, 0)

    keep(send, held)
    entries = [
        gate_entries(fields[15 + k], fields[16 + k], (1, 128)) for k in range(7)
    ]
    srow = lax.broadcasted_iota(jnp.int32, (8, 128), 0)
    bit1, bit2 = (srow >> 1) & 1, (srow >> 2) & 1
    low, up, down, high, flip = entries[0]
    d15 = jnp.where(bit1 == bit2, jnp.where(bit1 == 0, low, high), jnp.where(bit1 == 0, up, down))
    f15 = jnp.where(bit1 == bit2, 0.0, flip)
    below15 = jnp.where(bit1 == 0, f15, 0.0)
    above15 = jnp.where(bit1 == 0, 0.0, f15)
    low, up, down, high, flip = entries[1]
    d16_0 = jnp.where(bit2 == 0, low, down)
    f16_0 = jnp.where(bit2 == 0, 0.0, flip)
    d16_1 = jnp.where(bit2 == 0, up, high)
    f16_1 = jnp.where(bit2 == 0, flip, 0.0)
    arrived(send, held, 0)

    for c in range(n // 8):
        v = held[32 * c : 32 * (c + 1), :].reshape(4, 8, 128)
        v = v * d15 + pltpu.roll(v, 2, 1) * below15 + pltpu.roll(v, 6, 1) * above15
        v = v.reshape(2, 2, 8, 128)
        v0, v1 = v[:, 0], v[:, 1]
        u0 = v0 * d16_0 + pltpu.roll(v1, 4, 1) * f16_0
        u1 = v1 * d16_1 + pltpu.roll(v0, 4, 1) * f16_1
        v = jnp.stack([u0, u1], axis=1).reshape(32, 128)
        t_ref[32 * c : 32 * (c + 1), :] = mix(v, entries[2], 3)
    total = jnp.zeros((8, 128), jnp.float32)
    for h in range(2):
        v = jnp.concatenate(
            [t_ref[16 * g + 8 * h : 16 * g + 8 * h + 8, :] for g in range(4 * n // 16)], axis=0
        )
        for k in range(4):
            v = mix(v, entries[3 + k], 3 + k)
        total = total + jnp.sum((v * v).reshape(-1, 8, 128), axis=0)
        for g in range(4 * n // 16):
            back[16 * g + 8 * h : 16 * g + 8 * h + 8, :] = v[8 * g : 8 * (g + 1)]

    part_z[...] = jnp.sum(total, axis=0, keepdims=True)

    def small(source, target, slot, px, py, s_sem, r_sem):
        return pltpu.make_async_remote_copy(
            src_ref=source,
            dst_ref=target.at[slot],
            send_sem=s_sem,
            recv_sem=r_sem,
            device_id={"gx": px, "gy": py},
            device_id_type=MESH,
        )

    @pl.loop(1, n_z)
    def _(k):
        tz = (z + k) % n_z
        small(part_z, got_z, z, 2 * tz + core, gy, send_sems.at[2], got_z_sem.at[0]).start()

    got_z[z] = part_z[...]

    @pl.loop(0, n_z - 1)
    def _(t):
        tz = far_first(t)
        for i in range(plane):
            post(back, final, 1, tz, i)

    for i in range(plane):

        @pl.when(i != mine)
        def _():
            post(back, final, 1, z, i)

    keep(back, final)
    pltpu.make_async_copy(
        got_z.at[pl.ds(0, n_z - 1)], got_z.at[pl.ds(0, n_z - 1)], got_z_sem.at[0]
    ).wait()
    part_xc[...] = jnp.sum(got_z[...], axis=0)

    @pl.loop(1, 2 * n_x)
    def _(k):
        tc, tx = (core + k % 2) % 2, (gy + k // 2) % n_x
        small(part_xc, got_xc, mine, 2 * z + tc, tx, send_sems.at[3], got_xc_sem.at[0]).start()

    got_xc[mine] = part_xc[...]
    pltpu.make_async_copy(
        got_xc.at[pl.ds(0, 2 * n_x - 1)], got_xc.at[pl.ds(0, 2 * n_x - 1)], got_xc_sem.at[0]
    ).wait()
    summed = jnp.sum(jnp.sum(got_xc[...], axis=0), axis=1, keepdims=True)
    count = float(x_ref.shape[0] * x_ref.shape[1] * n)
    scale = lax.rsqrt(summed / count + EPSILON)
    arrived(back, final, 1)
    for n15 in range(2):
        for n7 in range(2):
            o_ref[pl.ds(n15 * 256 + n7, 128, stride=2), :] = (
                final[pl.ds(2 * n15 + n7, 128, stride=4), :] * scale
            )
    sent(send, held, 0)
    sent(back, final, 1)
    pltpu.make_async_copy(
        got_z.at[pl.ds(0, n_z - 1)], got_z.at[pl.ds(0, n_z - 1)], send_sems.at[2]
    ).wait()
    pltpu.make_async_copy(
        got_xc.at[pl.ds(0, 2 * n_x - 1)], got_xc.at[pl.ds(0, 2 * n_x - 1)], send_sems.at[3]
    ).wait()


def local(initial_state, fields, bond_order):
    amps = initial_state.shape[2]
    n = lax.axis_size("gx") * lax.axis_size("gy")
    n_z, n_xc = lax.axis_size("gx") // 2, 2 * lax.axis_size("gy")
    block = pltpu.VMEM((amps // 128, 128), jnp.float32)
    vmem, hbm = pl.BlockSpec(memory_space=pltpu.VMEM), pl.BlockSpec(memory_space=pltpu.HBM)
    pin = functools.partial(pltpu.with_memory_space_constraint, memory_space=pltpu.HBM)
    out = pl.pallas_call(
        kernel,
        out_shape=jax.ShapeDtypeStruct((amps // 128, 128), jnp.float32),
        in_specs=[hbm, hbm, hbm],
        out_specs=vmem,
        scratch_shapes=[
            pltpu.SMEM(fields.shape, jnp.float32),
            pltpu.SMEM(bond_order.shape, jnp.int32),
            block,
            block,
            block,
            block,
            block,
            block,
            pltpu.VMEM((1, 128), jnp.float32),
            pltpu.VMEM((1, 128), jnp.float32),
            pltpu.VMEM((n_z, 1, 128), jnp.float32),
            pltpu.VMEM((n_xc, 1, 128), jnp.float32),
            pltpu.SemaphoreType.DMA((4,)),
            pltpu.SemaphoreType.DMA((2,)),
            pltpu.SemaphoreType.DMA((1,)),
            pltpu.SemaphoreType.DMA((1,)),
            pltpu.SemaphoreType.DMA((3,)),
            pltpu.SemaphoreType.REGULAR((n_z + 1,)),
        ],
        compiler_params=pltpu.CompilerParams(
            collective_id=0, has_side_effects=True, vmem_limit_bytes=4 * 2**20
        ),
    )(
        pin(initial_state.reshape(amps // 128, 128)), pin(fields), pin(bond_order)
    )
    return out.reshape(initial_state.shape)


def solution(mesh):
    placed = (P(("groups", "gx"), "gy", None), P("groups"), P())
    return jax.shard_map(
        local,
        mesh=mesh,
        in_specs=placed,
        out_specs=P(("groups", "gx"), "gy", None),
        check_vma=False,
    )
```
